32 devices in a mesh: row: 4 (over y, x), col: 8 (over z, core).
Axes of the slice: x: 2, y: 2, z: 4, core: 2. Of those that a mesh axis runs over, the one named last changes fastest.
Arguments:
- tokens: bfloat16 [4096, 2048], P(('row', 'col')), may hold values from -6 to 6
- expert_ids: int32 [4096, 8], P(('row', 'col')), may hold values from 0 to 31, all different within a row; in each aligned block of 128 rows (0 to 127, 128 to 255, ...) at most 40 rows name the same one
- gate_probs: float32 [4096, 8], P(('row', 'col')), may hold values from 0.05 to 0.5
- w_gate: bfloat16 [32, 2048, 768], P(('row', 'col')), may hold values from -0.125 to 0.125
- w_up: bfloat16 [32, 2048, 768], P(('row', 'col')), may hold values from -0.125 to 0.125
- w_down: bfloat16 [32, 768, 2048], P(('row', 'col')), may hold values from -0.21875 to 0.21875
Outputs:
- mixed: bfloat16 [4096, 2048], P(('row', 'col'))
The draws below stay inside these ranges and needn't reach their ends.
Inputs may be any that keep to these rules, and one draw needn't show every extreme that they name: `expert_ids`: each row names 8 different experts; among the rows of one device (aligned blocks of 128 rows) no expert is named more than 40 times.
All inputs are finite; a program needn't handle non-finite values.
Results may differ from the reference program's by a relative error of at most 0.0058.
Values may be sent and summed in bfloat16 or wider, within the bound.
A program may use at most 128 MiB of HBM per device.

```python
import math
import jax
import jax.numpy as jnp
import numpy as np
from jax import lax

D = 2048
FF = 768
TOPK = 8
TOK_DEV = 128
EXPERTS = 32
TOKENS = 4096
SLOTS = 40
N_ROW = 4
N_COL = 8


def level_of(stream_key, extent, shards, smallest, high):
    def one(axis_at, blocks):
        draws = jax.random.uniform(jax.random.fold_in(jax.random.fold_in(stream_key, 6), axis_at), (blocks,), jnp.float32, smallest / len(shards), high / len(shards))
        return jnp.repeat(jnp.exp(draws), extent[axis_at] // blocks).reshape((-1,) + (1,) * (len(extent) - axis_at - 1))

    loudness = one(*shards[0])
    for cut in shards[1:]:
        loudness = loudness * one(*cut)
    return loudness


def shared_out(own_key, own, number, rows, count, top, most, slope):
    order = jax.random.permutation(own_key, count)
    crowded, ordinary = load_shares(count, rows * top, most, slope, True), load_shares(count, rows * top, most, slope, False)
    places = jnp.arange(count)

    def named(lengths, rotation):
        used = int((lengths > 0).sum())
        fixed = max(1, used // 4)
        shifted = fixed + (places - fixed + rotation * (used - fixed)) % max(1, count - fixed)
        return jnp.zeros((count,), jnp.int32).at[order[jnp.where(places < fixed, places, shifted)]].set(jnp.asarray(lengths, jnp.int32))

    lengths = jnp.where(number % 4 == 0, named(crowded, number // 4), named(ordinary, number - number // 4 - 1))
    mixed = jax.random.permutation(jax.random.fold_in(own, 3), count)
    source_of, taker = mixed[0:count // 2 * 2:2], mixed[1:count // 2 * 2:2]
    room = jnp.minimum(lengths[source_of] - 1, most - lengths[taker]) // 2
    room = jnp.where((source_of == order[0]) | (taker == order[0]) | (lengths[taker] == 0), 0, jnp.maximum(room, 0))
    shifted = jax.random.randint(jax.random.fold_in(own, 4), (count // 2,), 0, 1 << 20) % (room + 1)
    lengths = lengths.at[source_of].add(-shifted).at[taker].add(shifted)
    members = jnp.searchsorted(jnp.cumsum(lengths), jnp.arange(rows * top), side="right").astype(jnp.int32)
    listing = members.reshape(top, rows).T
    listing = listing[jax.random.permutation(jax.random.fold_in(own, 1), rows)]
    rotation = jax.random.randint(jax.random.fold_in(own, 2), (rows, 1), 0, top)
    return jnp.take_along_axis(listing, (jnp.arange(top)[None, :] + rotation) % top, axis=1)


def load_shares(number_of, total, most, slope, full):
    loads = [(1 << 20) // math.isqrt(rank ** slope) + 1 for rank in range(1, number_of + 1)]
    largest = most if full else min(most, max(-(-total // number_of), total * loads[0] // sum(loads)))
    least = 1 if total - largest >= number_of - 1 else 0
    counts, rest = [largest] + [least] * (number_of - 1), total - largest - least * (number_of - 1)
    while rest > 0:
        movable = [i for i in range(1, number_of) if counts[i] < largest] or [i for i in range(1, number_of) if counts[i] < most]
        whole, left = sum([loads[i] for i in movable]), rest
        for i in movable:
            addition = min(most - counts[i], max(1, left * loads[i] // whole), rest)
            counts[i] = counts[i] + addition
            rest = rest - addition
    return np.array(counts)


def gaussian(key, shape, deviation, bound, cuts=(), held_as=jnp.bfloat16):
    drawn = deviation * jax.random.normal(key, shape, jnp.float32)
    if cuts:
        drawn = drawn * level_of(key, shape, cuts, -0.22, 0.18)
    return jnp.clip(drawn, -bound, bound).astype(held_as)


def setup_inputs(seed: int = 0) -> dict:
    seeds = jax.random.split(jax.random.key(seed), 7)
    tokens = gaussian(seeds[0], (TOKENS, D), 1.0, 6.0, ((0, 32),))
    expert_ids_keys = jax.random.split(jax.random.fold_in(seeds[1], 1), TOKENS // TOK_DEV)
    expert_ids_turns = jax.random.permutation(jax.random.fold_in(seeds[1], 3), TOKENS // TOK_DEV)
    expert_ids = jax.vmap(lambda own, number: shared_out(jax.random.fold_in(seeds[1], 2), own, number, TOK_DEV, EXPERTS, TOPK, SLOTS, 2))(expert_ids_keys, expert_ids_turns).reshape((TOKENS, TOPK))
    gate_probs = jnp.clip(0.05 + 0.45 * jax.random.uniform(seeds[2], (TOKENS, TOPK), jnp.float32) ** level_of(seeds[2], (TOKENS, TOPK), ((0, 32),), -0.2, 0.2), 0.05, 0.5)
    w_gate = gaussian(seeds[3], (EXPERTS, D, FF), D ** -0.5, 0.125, ((0, 32),))
    w_up = gaussian(seeds[4], (EXPERTS, D, FF), D ** -0.5, 0.125, ((0, 32),))
    w_down = gaussian(seeds[5], (EXPERTS, FF, D), FF ** -0.5, 0.21875, ((0, 32),))
    return dict(tokens=tokens, expert_ids=expert_ids, gate_probs=gate_probs, w_gate=w_gate, w_up=w_up, w_down=w_down)


def reference(tokens, expert_ids, gate_probs, w_gate, w_up, w_down):
    sources = N_ROW * N_COL
    flat_ids = expert_ids.reshape(sources, TOK_DEV * TOPK)
    onehot = (flat_ids[:, :, None] == jnp.arange(EXPERTS, dtype=jnp.int32)[None, None, :]).astype(jnp.int32)
    rank = jnp.sum((jnp.cumsum(onehot, axis=1) - 1) * onehot, axis=2).astype(jnp.int32)
    source = jnp.arange(sources, dtype=jnp.int32)[:, None]
    position = (flat_ids * (sources * SLOTS) + source * SLOTS + rank).reshape(-1).astype(jnp.int32)
    token_of = (jnp.arange(TOKENS * TOPK, dtype=jnp.int32) // TOPK).astype(jnp.int32)
    owner = jnp.full((EXPERTS * sources * SLOTS,), -1, jnp.int32).at[position].set(token_of)
    owner = owner.reshape(EXPERTS, sources * SLOTS)

    def one_expert(index):
        picks = owner[index]
        rows = tokens[jnp.maximum(picks, 0)]
        rows = jnp.where((picks >= 0)[:, None], rows, jnp.zeros((), tokens.dtype))
        gate = jnp.dot(rows, w_gate[index], preferred_element_type=jnp.float32)
        up = jnp.dot(rows, w_up[index], preferred_element_type=jnp.float32)
        hidden = (jax.nn.silu(gate) * up).astype(jnp.bfloat16)
        return jnp.dot(hidden, w_down[index], preferred_element_type=jnp.float32).astype(jnp.bfloat16)

    outputs = lax.map(one_expert, jnp.arange(EXPERTS, dtype=jnp.int32))
    picked = outputs.reshape(-1, D)[position].reshape(TOKENS, TOPK, D).astype(jnp.float32)
    mixed = jnp.sum(gate_probs.astype(jnp.float32)[:, :, None] * picked, axis=1)
    return mixed.astype(jnp.bfloat16)
```

```python
import functools
import math

import jax
import jax.numpy as jnp
from jax import lax
from jax.experimental import pallas as pl
from jax.experimental.pallas import tpu as pltpu
from jax.sharding import PartitionSpec as P

MESH = pl.DeviceIdType.MESH
BF16 = jnp.bfloat16
F32 = jnp.float32
PIECES = 2
OWN, PAR = 0, 1


def flip(r, j):
    out, bit = r, 1
    while bit <= j:
        if j & bit:
            out = out + bit * (1 - 2 * ((r // bit) % 2))
        bit *= 2
    return out


def plan(chunks, per, chips):
    hops = range(1, chips)
    if per > 1 or chunks < 4:
        every = range(chunks)
        return (
            [("D", i) for i in every] + [("F", d, "all") for d in range(chips)]
            + [("P", i) for i in every] + [("X", i, 1) for i in every]
            + [("C", o, i) for o in (OWN, PAR) for i in every]
            + [("R", o, k) for o in (OWN, PAR) for k in hops] + [("H", PAR), ("H", OWN)]
        )
    last = chunks - 1
    seq = [("D", 0), ("D", 1), ("F", 0, "all"), ("P", 0), ("X", 0, 1)]
    for i in range(2, chunks):
        seq += [("D", i), ("X", i - 1, 0)]
        if i == 2:
            seq += [("C", OWN, 0), ("C", PAR, 0)]
        else:
            seq += [("C", OWN, i - 2), ("R", OWN, i - 2)]
    seq += [("F", d, "mid") for d in range(1, last)]
    seq += [("X", last, 0), ("C", OWN, last - 1), ("R", OWN, last - 1), ("F", last, "mid")]
    for i in hops:
        seq += [("F", i, "end"), ("P", i), ("X", i, 2)]
        if i == 1:
            seq += [("C", OWN, last), ("R", OWN, last)]
        seq += [("C", PAR, i), ("R", PAR, i)]
    return seq + [("H", PAR), ("H", OWN)]


def moe_kernel(
    rows, cols, slots, group, pieces,
    ids_in, probs_in, tok_in, wg_in, wu_in, wd_in, out_ref,
    ids_v, probs_v, meta, tok, wg, wu, wd, disp, comb, hid, xs, xr, yr, pr, zr, dr,
    load_sem, m_send, m_recv, pt_sem, ztok_send, ztok_recv, ctok_send, ctok_recv,
    x_send, x_recv, y_send, y_recv, p_send, p_recv, z_send, z_recv, d_send, d_recv,
):
    r = lax.axis_index("row")
    c = lax.axis_index("col")
    chips = cols // 2
    chip, core = c // 2, c % 2
    mate = 2 * chip + (1 - core)
    far = rows - 1
    partner = flip(r, far)
    count, width = tok_in.shape
    choices = ids_in.shape[0]
    per = group // 2
    chunks = chips // per
    part = group * slots
    near = far * part
    hidden = wg.shape[1]
    f_tile = math.gcd(hidden, 256)
    d_tile = math.gcd(width // pieces, 512)
    piece = width // pieces

    def remote(src, dst, send, recv, row, col):
        return pltpu.make_async_remote_copy(
            src_ref=src, dst_ref=dst, send_sem=send, recv_sem=recv,
            device_id=(row, col), device_id_type=MESH,
        )

    short = jnp.minimum(chip, chips - 1 - chip)
    side = jnp.where(2 * chip < chips, 1, -1)
    order, signs = [chip], [None]
    for p in range(1, chips):
        both = p <= 2 * short
        sign = jnp.where(both, 1 if p % 2 else -1, side)
        dist = jnp.where(both, (p + 1) // 2, p - short)
        order.append(chip + sign * dist)
        signs.append(sign)

    load_tok = pltpu.make_async_copy(tok_in, tok.at[OWN, chip, 0], load_sem.at[0])
    load_ids = pltpu.make_async_copy(ids_in, ids_v, load_sem.at[1])
    load_probs = pltpu.make_async_copy(probs_in, probs_v, load_sem.at[5])
    load_w = [
        pltpu.make_async_copy(wg_in.at[0], wg, load_sem.at[2]),
        pltpu.make_async_copy(wu_in.at[0], wu, load_sem.at[3]),
        pltpu.make_async_copy(wd_in.at[0], wd, load_sem.at[4]),
    ]
    load_tok.start()
    load_ids.start()
    load_probs.start()

    barrier = pltpu.get_barrier_semaphore()
    for d in range(1, cols):
        for row in (r, partner):
            pl.semaphore_signal(
                barrier, inc=1, device_id=(row, (c + d) % cols), device_id_type=MESH
            )
    for j in range(1, rows):
        pl.semaphore_signal(barrier, inc=1, device_id=(flip(r, j), c), device_id_type=MESH)
    pl.semaphore_wait(barrier, 2 * (cols - 1) + rows - 1)

    def hop(o, q, send, to):
        return remote(
            tok.at[o, q, 0], tok.at[o, q, 0], ztok_send.at[o, send], ztok_recv.at[o, q],
            r, 2 * ((to + chips) % chips) + core,
        )

    def onward(o, p, act):
        if p == 0:
            @pl.when(chip > 0)
            def _():
                act(hop(o, chip, 0, chip - 1))

            @pl.when(chip < chips - 1)
            def _():
                act(hop(o, chip, chips, chip + 1))
        else:
            to = chip - signs[p]

            @pl.when((to >= 0) & (to < chips))
            def _():
                act(hop(o, order[p], p, to))

    ctok = [
        [
            remote(
                tok.at[o, q, 0], tok.at[o, q, 1], ctok_send.at[o, p], ctok_recv.at[o, p], r, mate
            )
            for p, q in enumerate(order)
        ]
        for o in (OWN, PAR)
    ]
    ptok = remote(tok.at[OWN, chip, 0], tok.at[PAR, chip, 0], pt_sem.at[0], pt_sem.at[1], partner, c)

    def routing(o, d, t, slot):
        dist, other = d // 2, d % 2
        to = 2 * t + (core if other == 0 else 1 - core)
        return remote(
            meta.at[OWN, chip, 0], meta.at[o, slot, other],
            m_send.at[o, d], m_recv.at[o, slot, other], partner if o else r, to,
        )

    load_tok.wait()
    ctok[OWN][0].start()
    onward(OWN, 0, lambda copy: copy.start())
    load_ids.wait()
    load_probs.wait()
    meta[OWN, chip, 0, :choices] = ids_v[...].astype(F32)
    meta[OWN, chip, 0, choices:] = probs_v[...]
    for o in (OWN, PAR):
        for d in range(1 - o, cols):
            routing(o, d, (chip + d // 2) % chips, chip).start()
    ptok.start()
    for copy in load_w:
        copy.start()
    earlier = (
        lax.broadcasted_iota(jnp.int32, (count, count), 0)
        < lax.broadcasted_iota(jnp.int32, (count, count), 1)
    ).astype(BF16)
    slot_of = lax.broadcasted_iota(jnp.int32, (part, count), 0).astype(F32)
    lane_rows = 16
    row_id = lax.broadcasted_iota(jnp.int32, (lane_rows, count), 0)

    def route(o, i):
        for s in range(group):
            q = order[i * per + s // 2]
            ids = meta[o, q, s % 2, :choices].astype(jnp.int32)
            probs = meta[o, q, s % 2, choices:]
            named = jnp.zeros((lane_rows, count), F32)
            weights = []
            span = range(far) if o == OWN else [0]
            for j in span:
                expert = flip(r, j) * cols + c
                hit = (ids == expert).astype(F32)
                named = jnp.where(row_id == j, jnp.sum(hit, axis=0, keepdims=True), named)
                weights.append(jnp.sum(hit * probs, axis=0, keepdims=True))
            rank = jnp.dot(named.astype(BF16), earlier, preferred_element_type=F32)
            key = jnp.where(named > 0.5, rank + float(s * slots), -1.0)
            for j in span:
                one = (slot_of == key[j:j + 1, :]).astype(F32)
                at = pl.ds((j if o == OWN else far) * part, part)
                disp[at, s * count:(s + 1) * count] = one.astype(BF16)
                comb[i, at, s * count:(s + 1) * count] = (one * weights[j]).astype(BF16)

    x_out, y_out = {}, {}

    def arrive(o, d):
        if o == PAR and d == 0:
            ptok.wait_recv()
        else:
            hop(o, order[d], d, chip).wait_recv()
        onward(o, d, lambda copy: copy.start())
        ctok[o][d].start()

    def settle(o, i):
        for d in range(i * per, (i + 1) * per):
            for other in range(1 if o == OWN and d == 0 else 0, 2):
                routing(o, other, order[d], order[d]).wait_recv()
        route(o, i)
        for d in range(i * per, (i + 1) * per):
            ctok[o][d].wait_recv()

    def blocks(o, i, at):
        return jnp.concatenate(
            [tok[o, q, :, :, at].reshape(2 * count, d_tile) for q in order[i * per:(i + 1) * per]]
        )

    def dispatch(i):
        for d in range(i * per, (i + 1) * per):
            if d > 0:
                arrive(OWN, d)
        settle(OWN, i)

        def tile(n, _):
            at = pl.ds(pl.multiple_of(n * d_tile, d_tile), d_tile)
            res = jnp.dot(disp[:near], blocks(OWN, i, at), preferred_element_type=F32).astype(BF16)
            xr[i, 0, :, at] = res[:part]
            xs[i, :, :, at] = res[part:].reshape(far - 1, part, d_tile)
            return 0

        lax.fori_loop(0, width // d_tile, tile, 0)
        for j in range(1, far):
            copy = remote(
                xs.at[i, j - 1], xr.at[i, j], x_send.at[i, j], x_recv.at[i, j], flip(r, j), c
            )
            copy.start()
            x_out[i, j] = copy

    def dispatch_partner(i):
        settle(PAR, i)

        def tile(n, _):
            at = pl.ds(pl.multiple_of(n * d_tile, d_tile), d_tile)
            xr[i, far, :, at] = jnp.dot(
                disp[near:], blocks(PAR, i, at), preferred_element_type=F32
            ).astype(BF16)
            return 0

        lax.fori_loop(0, width // d_tile, tile, 0)

    def experts(i, lo, hi, first):
        if lo == 0:
            for j in range(1, far):
                x_out[i, j].wait()
        if first:
            for copy in load_w:
                copy.wait()
        size = (hi - lo) * part

        def up_tile(n, _):
            at = pl.ds(pl.multiple_of(n * f_tile, f_tile), f_tile)
            x = xr[i, lo:hi].reshape(size, width)
            gate = jnp.dot(x, wg[:, at], preferred_element_type=F32)
            up = jnp.dot(x, wu[:, at], preferred_element_type=F32)
            hid[:size, at] = (gate / (1.0 + jnp.exp(-gate)) * up).astype(BF16)
            return 0

        lax.fori_loop(0, hidden // f_tile, up_tile, 0)

        def down_tile(n, _):
            at = pl.ds(pl.multiple_of(n * d_tile, d_tile), d_tile)
            res = jnp.dot(hid[:size], wd[:, at], preferred_element_type=F32).astype(BF16)
            if lo == 0:
                yr[i, 0, :, at] = res[:part]
                xs[i, :, :, at] = res[part:near].reshape(far - 1, part, d_tile)
            if hi == rows:
                yr[i, far, :, at] = res[size - part:]
            return 0

        for h in range(pieces):
            at = pl.ds(h * piece, piece)
            lax.fori_loop(h * piece // d_tile, (h + 1) * piece // d_tile, down_tile, 0)
            if lo == 0:
                for j in range(1, far):
                    copy = remote(
                        xs.at[i, j - 1, :, at], yr.at[i, j, :, at],
                        y_send.at[i, j, h], y_recv.at[i, j, h], flip(r, j), c,
                    )
                    copy.start()
                    y_out[i, j, h] = copy

    def mate_copy(o, q, h):
        at = pl.ds(h * piece, piece)
        return remote(
            tok.at[o, q, 1, :, at], pr.at[o, q, :, at],
            p_send.at[o, q, h], p_recv.at[o, q, h], r, mate,
        )

    def combine(o, i):
        for d in range(i * per, (i + 1) * per):
            onward(o, d, lambda copy: copy.wait_send())
            ctok[o][d].wait_send()
            if o == OWN and d == 0:
                ptok.wait_send()
        lo, hi = (0, far) if o == OWN else (far, rows)
        for h in range(pieces):
            if o == OWN:
                for j in range(1, far):
                    y_out[i, j, h].wait()

            def tile(n, _):
                at = pl.ds(pl.multiple_of(n * d_tile, d_tile), d_tile)
                y = yr[i, lo:hi, :, at].reshape((hi - lo) * part, d_tile)
                res = lax.dot_general(
                    comb[i, lo * part:hi * part], y, (((0,), (0,)), ((), ())),
                    preferred_element_type=F32,
                ).astype(BF16)
                for p in range(per):
                    q = order[i * per + p]
                    tok[o, q, 0, :, at] = res[2 * p * count:(2 * p + 1) * count]
                    tok[o, q, 1, :, at] = res[(2 * p + 1) * count:(2 * p + 2) * count]
                return 0

            lax.fori_loop(h * piece // d_tile, (h + 1) * piece // d_tile, tile, 0)
            for d in range(i * per, (i + 1) * per):
                mate_copy(o, order[d], h).start()

    def chain(o, t, h, step):
        at = pl.ds(h * piece, piece)
        to = (chip + step + chips) % chips
        slot = jnp.where(to == t, chips, t) if step > 0 else t
        return remote(
            tok.at[o, t, 0, :, at], zr.at[o, slot, :, at],
            z_send.at[o, t, h], z_recv.at[o, slot, h], r, 2 * to + core,
        )

    def landed(o, slot, h):
        at = pl.ds(h * piece, piece)
        remote(
            tok.at[o, chip, 0, :, at], zr.at[o, slot, :, at],
            z_send.at[o, chip, h], z_recv.at[o, slot, h], r, mate,
        ).wait_recv()
        return zr[o, slot, :, at].astype(F32)

    def both_cores(o, q, h):
        at = pl.ds(h * piece, piece)
        return tok[o, q, 0, :, at].astype(F32) + pr[o, q, :, at].astype(F32)

    def reduce(o, k):
        for h in range(pieces):
            at = pl.ds(h * piece, piece)
            for step, t, edge in ((1, k, 0), (-1, chips - 1 - k, chips - 1)):
                @pl.when((t - chip) * step > 0)
                def _():
                    mate_copy(o, t, h).wait()

                    @pl.when(chip == edge)
                    def _():
                        tok[o, t, 0, :, at] = both_cores(o, t, h).astype(BF16)

                    @pl.when(chip != edge)
                    def _():
                        tok[o, t, 0, :, at] = (landed(o, t, h) + both_cores(o, t, h)).astype(BF16)

                    chain(o, t, h, step).start()

    def back(h):
        at = pl.ds(h * piece, piece)
        return remote(
            tok.at[PAR, chip, 0, :, at], dr.at[:, at], d_send.at[h], d_recv.at[h], partner, c
        )

    def home(o):
        for h in range(pieces):
            at = pl.ds(h * piece, piece)
            mate_copy(o, chip, h).wait()

            def finish(*slots_in):
                total = both_cores(o, chip, h)
                for slot in slots_in:
                    total = total + landed(o, slot, h)
                if o == PAR:
                    tok[PAR, chip, 0, :, at] = total.astype(BF16)
                    back(h).start()
                else:
                    back(h).wait_recv()
                    out_ref[:, at] = (total + dr[:, at].astype(F32)).astype(BF16)

            pl.when(chip == 0)(lambda: finish(chip))
            pl.when(chip == chips - 1)(lambda: finish(chips))
            pl.when((chip > 0) & (chip < chips - 1))(lambda: finish(chip, chips))

    edge_chip = (chip == 0) | (chip == chips - 1)
    for step in plan(chunks, per, chips):
        kind = step[0]
        if kind == "D":
            dispatch(step[1])
        elif kind == "F":
            if step[2] == "all":
                arrive(PAR, step[1])
            else:
                pl.when(edge_chip if step[2] == "end" else jnp.logical_not(edge_chip))(
                    functools.partial(arrive, PAR, step[1])
                )
        elif kind == "P":
            dispatch_partner(step[1])
        elif kind == "X":
            lo, hi = ((0, far), (0, rows), (far, rows))[step[2]]
            experts(step[1], lo, hi, step == ("X", 0, 1))
        elif kind == "C":
            combine(step[1], step[2])
        elif kind == "R":
            reduce(step[1], step[2])
        else:
            home(step[1])

    for o in (OWN, PAR):
        for d in range(1 - o, cols):
            routing(o, d, (chip + d // 2) % chips, chip).wait_send()
        for d in range(1, chips):
            for h in range(pieces):
                chain(o, order[d], h, 1).wait_send()
    for h in range(pieces):
        back(h).wait_send()


def body(tokens, expert_ids, gate_probs, w_gate, w_up, w_down):
    count, choices = expert_ids.shape
    width = tokens.shape[1]
    hidden = w_gate.shape[2]
    rows = lax.axis_size("row")
    cols = lax.axis_size("col")
    slots = 5 * count * choices // (4 * rows * cols * w_gate.shape[0])
    group = 2
    while group * slots % 16:
        group *= 2
    chips = cols // 2
    chunks = chips // (group // 2)
    part = group * slots
    any_spec = pl.BlockSpec(memory_space=pl.ANY)
    dma = pltpu.SemaphoreType.DMA
    scratch = [
        pltpu.VMEM((choices, count), jnp.int32),
        pltpu.VMEM((choices, count), F32),
        pltpu.VMEM((2, chips, 2, 2 * choices, count), F32),
        pltpu.VMEM((2, chips, 2, count, width), BF16),
        pltpu.VMEM((width, hidden), BF16),
        pltpu.VMEM((width, hidden), BF16),
        pltpu.VMEM((hidden, width), BF16),
        pltpu.VMEM((rows * part, group * count), BF16),
        pltpu.VMEM((chunks, rows * part, group * count), BF16),
        pltpu.VMEM((rows * part, hidden), BF16),
        pltpu.VMEM((chunks, rows - 2, part, width), BF16),
        pltpu.VMEM((chunks, rows, part, width), BF16),
        pltpu.VMEM((chunks, rows, part, width), BF16),
        pltpu.VMEM((2, chips, count, width), BF16),
        pltpu.VMEM((2, chips + 1, count, width), BF16),
        pltpu.VMEM((count, width), BF16),
        dma((6,)),
        dma((2, cols)), dma((2, chips, 2)),
        dma((2,)),
        dma((2, chips + 1)), dma((2, chips)),
        dma((2, chips)), dma((2, chips)),
        dma((chunks, rows)), dma((chunks, rows)),
        dma((chunks, rows, PIECES)), dma((chunks, rows, PIECES)),
        dma((2, chips, PIECES)), dma((2, chips, PIECES)),
        dma((2, chips, PIECES)), dma((2, chips + 1, PIECES)),
        dma((PIECES,)), dma((PIECES,)),
    ]
    return pl.pallas_call(
        functools.partial(moe_kernel, rows, cols, slots, group, PIECES),
        out_shape=jax.ShapeDtypeStruct((count, width), BF16),
        in_specs=[any_spec] * 6,
        out_specs=pl.BlockSpec(memory_space=pltpu.VMEM),
        scratch_shapes=scratch,
        compiler_params=pltpu.CompilerParams(
            collective_id=0, has_side_effects=True, vmem_limit_bytes=67043328
        ),
    )(expert_ids.T, gate_probs.T, tokens, w_gate, w_up, w_down)


def solution(mesh):
    in_specs = (
        P(("row", "col"), None),
        P(("row", "col"), None),
        P(("row", "col"), None),
        P(("row", "col"), None, None),
        P(("row", "col"), None, None),
        P(("row", "col"), None, None),
    )
    out_specs = P(("row", "col"), None)
    return jax.shard_map(body, mesh=mesh, in_specs=in_specs, out_specs=out_specs, check_vma=False)
```

```python
import functools
import math

import jax
import jax.numpy as jnp
from jax import lax
from jax.experimental import pallas as pl
from jax.experimental.pallas import tpu as pltpu
from jax.sharding import PartitionSpec as P

MESH = pl.DeviceIdType.MESH
BF16 = jnp.bfloat16
F32 = jnp.float32
PIECES = 4
HALVES = 2
OWN, PAR = 0, 1


def flip(r, j):
    out, bit = r, 1
    while bit <= j:
        if j & bit:
            out = out + bit * (1 - 2 * ((r // bit) % 2))
        bit *= 2
    return out


def staged(chips, per):
    return per == 1 and chips == 4


def plan(chips, per):
    hops = range(1, chips)
    every = range(chips // per)
    if not staged(chips, per):
        return (
            [("A", OWN, d, "all") for d in hops] + [("D", i) for i in every]
            + [step for i in every for step in (("X", i, 0), ("Y", i))]
            + [("C", i, "all") for i in every] + [("R", k) for k in hops]
            + [("H", OWN, "all")]
        )
    return [
        ("D", 0), ("S", 0), ("A", OWN, 1, "all"), ("A", OWN, 2, "mid"), ("D", 1), ("S", 1),
        ("X", 0, 0), ("X", 1, 0), ("Y", 1),
        ("A", OWN, 3, "mid"), ("A", OWN, 2, "end"), ("D", 2),
        ("A", PAR, 0, "all"), ("P", 0), ("CR", 1), ("A", OWN, 3, "end"), ("D", 3),
        ("A", PAR, 1, "mid"), ("P", 1), ("X", 2, 0), ("Y", 2), ("X", 1, 1), ("X", 0, 1),
        ("A", PAR, 2, "mid"), ("P", 2), ("X", 2, 1), ("X", 3, 0), ("Y", 3), ("Y", 0),
        ("CP", 2), ("CP", 0), ("CP", 1), ("CR", 2),
        ("H", PAR, "mid"), ("C", 0, "mid"), ("CR", 3), ("H", PAR, "end"), ("C", 0, "end"),
        ("H", OWN, "all"),
    ]


def moe_kernel(
    rows, cols, slots, group, pieces,
    ids_in, probs_in, tok_in, wg_in, wu_in, wd_in, out_ref,
    ids_v, probs_v, meta, tok, wg, wu, wd, disp, comb, hid, xs, xr, yr, pr, zr, es, pz, dr,
    load_sem, m_send, m_recv, pt_send, pt_recv, ztok_send, ztok_recv, ctok_send, ctok_recv,
    x_send, x_recv, y_send, y_recv, p_send, p_recv, z_send, z_recv,
    e_send, e_recv, q_send, q_recv, d_send, d_recv,
):
    r = lax.axis_index("row")
    c = lax.axis_index("col")
    chips = cols // 2
    chip, core = c // 2, c % 2
    mate = 2 * chip + (1 - core)
    far = rows - 1
    partner = flip(r, far)
    count, width = tok_in.shape
    choices = ids_in.shape[0]
    per = group // 2
    chunks = chips // per
    part = group * slots
    shared = staged(chips, per)
    modes = (OWN, PAR) if shared else (OWN,)
    reach = [far if shared and i < chunks - 1 else rows for i in range(chunks)]
    hidden = wg.shape[1]
    f_tile = math.gcd(hidden, 256)
    d_tile = math.gcd(width // pieces, 512)
    piece = width // pieces
    half = width // HALVES

    def remote(src, dst, send, recv, row, col):
        return pltpu.make_async_remote_copy(
            src_ref=src, dst_ref=dst, send_sem=send, recv_sem=recv,
            device_id=(row, col), device_id_type=MESH,
        )

    short = jnp.minimum(chip, chips - 1 - chip)
    side = jnp.where(2 * chip < chips, 1, -1)
    inner = 2 * (chip + side) + core
    outer = 2 * ((chip - side + chips) % chips) + core
    edge = short == 0
    order, signs = [chip], [None]
    for p in range(1, chips):
        both = p <= 2 * short
        sign = jnp.where(both, side if p % 2 else -side, side)
        dist = jnp.where(both, (p + 1) // 2, p - short)
        order.append(chip + sign * dist)
        signs.append(sign)

    def on_edge(act):
        pl.when(edge)(act)

    def on_mid(act):
        pl.when(jnp.logical_not(edge))(act)

    load_tok = pltpu.make_async_copy(tok_in, tok.at[OWN, chip, 0], load_sem.at[0])
    load_ids = pltpu.make_async_copy(ids_in, ids_v, load_sem.at[1])
    load_probs = pltpu.make_async_copy(probs_in, probs_v, load_sem.at[5])
    load_w = [
        pltpu.make_async_copy(wg_in.at[0], wg, load_sem.at[2]),
        pltpu.make_async_copy(wu_in.at[0], wu, load_sem.at[3]),
        pltpu.make_async_copy(wd_in.at[0], wd, load_sem.at[4]),
    ]
    load_tok.start()
    load_ids.start()
    load_probs.start()

    barrier = pltpu.get_barrier_semaphore()
    for d in range(1, cols):
        for row in (r, partner)[:len(modes)]:
            pl.semaphore_signal(
                barrier, inc=1, device_id=(row, (c + d) % cols), device_id_type=MESH
            )
    for j in range(1, rows):
        pl.semaphore_signal(barrier, inc=1, device_id=(flip(r, j), c), device_id_type=MESH)
    pl.semaphore_wait(barrier, len(modes) * (cols - 1) + rows - 1)

    def hop(o, q, send, to, h):
        at = pl.ds(h * half, half)
        return remote(
            tok.at[o, q, 0, :, at], tok.at[o, q, 0, :, at],
            ztok_send.at[o, send, h], ztok_recv.at[o, q, h],
            r, 2 * ((to + chips) % chips) + core,
        )

    def onward(o, p, h, act):
        if o == PAR:
            if p == 0:
                act(hop(PAR, chip, 0, chip + side, h))
        elif p == 0:
            @pl.when(chip > 0)
            def _():
                act(hop(OWN, chip, 0, chip - 1, h))

            @pl.when(chip < chips - 1)
            def _():
                act(hop(OWN, chip, chips, chip + 1, h))
        else:
            to = chip - signs[p]

            @pl.when((to >= 0) & (to < chips))
            def _():
                act(hop(OWN, order[p], p, to, h))

    def swap(o, p):
        return remote(
            tok.at[o, order[p], 0], tok.at[o, order[p], 1],
            ctok_send.at[o, p], ctok_recv.at[o, p], r, mate,
        )

    def share(h):
        at = pl.ds(h * half, half)
        return remote(
            tok.at[OWN, chip, 0, :, at], tok.at[PAR, chip, 0, :, at],
            pt_send.at[h], pt_recv.at[h], partner, c,
        )

    def routing(o, d, t, slot):
        dist, other = d // 2, d % 2
        to = 2 * t + (core if other == 0 else 1 - core)
        return remote(
            meta.at[OWN, chip, 0], meta.at[o, slot, other],
            m_send.at[o, d], m_recv.at[o, slot, other], partner if o else r, to,
        )

    load_tok.wait()
    swap(OWN, 0).start()
    for h in range(HALVES):
        onward(OWN, 0, h, lambda copy: copy.start())
    load_ids.wait()
    load_probs.wait()
    meta[OWN, chip, 0, :choices] = ids_v[...].astype(F32)
    meta[OWN, chip, 0, choices:] = probs_v[...]
    for o in modes:
        for d in range(1 - o, cols):
            routing(o, d, (chip + d // 2) % chips, chip).start()
    for copy in load_w:
        copy.start()
    earlier = (
        lax.broadcasted_iota(jnp.int32, (count, count), 0)
        < lax.broadcasted_iota(jnp.int32, (count, count), 1)
    ).astype(BF16)
    slot_of = lax.broadcasted_iota(jnp.int32, (part, count), 0).astype(F32)
    lane_rows = 16
    row_id = lax.broadcasted_iota(jnp.int32, (lane_rows, count), 0)

    def route(o, i, base, experts_of):
        for s in range(group):
            q = order[i * per + s // 2]
            ids = meta[o, q, s % 2, :choices].astype(jnp.int32)
            probs = meta[o, q, s % 2, choices:]
            named = jnp.zeros((lane_rows, count), F32)
            weights = []
            for j, expert in enumerate(experts_of):
                hit = (ids == expert).astype(F32)
                named = jnp.where(row_id == j, jnp.sum(hit, axis=0, keepdims=True), named)
                weights.append(jnp.sum(hit * probs, axis=0, keepdims=True))
            rank = jnp.dot(named.astype(BF16), earlier, preferred_element_type=F32)
            key = jnp.where(named > 0.5, rank + float(s * slots), -1.0)
            for j in range(len(experts_of)):
                one = (slot_of == key[j:j + 1, :]).astype(F32)
                at = pl.ds((base + j) * part, part)
                disp[at, s * count:(s + 1) * count] = one.astype(BF16)
                comb[i, at, s * count:(s + 1) * count] = (one * weights[j]).astype(BF16)

    x_out, y_out = {}, {}

    def arrive(o, d):
        for h in range(HALVES):
            if o == PAR and d == 0:
                share(h).wait_recv()
            else:
                hop(o, order[d], d, chip, h).wait_recv()
            onward(o, d, h, lambda copy: copy.start())
        swap(o, d).start()

    def heard(o, i):
        for d in range(i * per, (i + 1) * per):
            for other in range(1 if o == OWN and d == 0 else 0, 2):
                routing(o, other, order[d], order[d]).wait_recv()

    def blocks(o, i, at):
        return jnp.concatenate(
            [tok[o, q, :, :, at].reshape(2 * count, d_tile) for q in order[i * per:(i + 1) * per]]
        )

    def dispatch(i):
        heard(OWN, i)
        route(OWN, i, 0, [flip(r, j) * cols + c for j in range(reach[i])])
        for d in range(i * per, (i + 1) * per):
            swap(OWN, d).wait_recv()
        near = reach[i] * part

        def tile(n, _):
            at = pl.ds(pl.multiple_of(n * d_tile, d_tile), d_tile)
            res = jnp.dot(disp[:near], blocks(OWN, i, at), preferred_element_type=F32).astype(BF16)
            xr[i, 0, :, at] = res[:part]
            xs[i, :reach[i] - 1, :, at] = res[part:].reshape(reach[i] - 1, part, d_tile)
            return 0

        lax.fori_loop(0, width // d_tile, tile, 0)
        for j in range(1, reach[i]):
            copy = remote(
                xs.at[i, j - 1], xr.at[i, j], x_send.at[i, j], x_recv.at[i, j], flip(r, j), c
            )
            copy.start()
            x_out[i, j] = copy

    def lent(i):
        return remote(es.at[i], xr.at[i + 1, far], e_send.at[i], e_recv.at[i], r, outer)

    def repaid(i):
        return remote(
            yr.at[i + 1, far], yr.at[i, rows], q_send.at[i], q_recv.at[i], r, inner
        )

    def dispatch_partner(i):
        def work(lend):
            heard(PAR, i)
            mine = [r * cols + c] + ([r * cols + outer] if lend else [])
            route(PAR, i, far, mine)
            swap(PAR, i).wait_recv()

            def tile(n, _):
                at = pl.ds(pl.multiple_of(n * d_tile, d_tile), d_tile)
                res = jnp.dot(
                    disp[far * part:(far + len(mine)) * part], blocks(PAR, i, at),
                    preferred_element_type=F32,
                ).astype(BF16)
                xr[i, far, :, at] = res[:part]
                if lend:
                    es[i, :, at] = res[part:]
                return 0

            lax.fori_loop(0, width // d_tile, tile, 0)
            if lend:
                lent(i).start()

        on_mid(lambda: work(i < 2))
        on_edge(lambda: heard(PAR, i) if i else work(False))

    def experts(i, lo, hi, first):
        if lo == 0:
            for j in range(1, hi):
                x_out[i, j].wait()
        elif i:
            on_edge(lambda: lent(i - 1).wait_recv())
        if first:
            for copy in load_w:
                copy.wait()
        size = (hi - lo) * part

        def up_tile(n, _):
            at = pl.ds(pl.multiple_of(n * f_tile, f_tile), f_tile)
            x = xr[i, lo:hi].reshape(size, width)
            gate = jnp.dot(x, wg[:, at], preferred_element_type=F32)
            up = jnp.dot(x, wu[:, at], preferred_element_type=F32)
            hid[:size, at] = (gate / (1.0 + jnp.exp(-gate)) * up).astype(BF16)
            return 0

        lax.fori_loop(0, hidden // f_tile, up_tile, 0)

        def down_tile(n, _):
            at = pl.ds(pl.multiple_of(n * d_tile, d_tile), d_tile)
            res = jnp.dot(hid[:size], wd[:, at], preferred_element_type=F32).astype(BF16)
            if lo == 0:
                yr[i, 0, :, at] = res[:part]
                xs[i, :hi - 1, :, at] = res[part:].reshape(hi - 1, part, d_tile)
            else:
                yr[i, far, :, at] = res
            return 0

        lax.fori_loop(0, width // d_tile, down_tile, 0)
        if lo and i:
            on_edge(lambda: repaid(i - 1).start())

    def reply(i):
        for h in range(pieces):
            at = pl.ds(h * piece, piece)
            for j in range(1, reach[i]):
                copy = remote(
                    xs.at[i, j - 1, :, at], yr.at[i, j, :, at],
                    y_send.at[i, j, h], y_recv.at[i, j, h], flip(r, j), c,
                )
                copy.start()
                y_out[i, j, h] = copy

    def mate_copy(o, q, h):
        at = pl.ds(h * piece, piece)
        return remote(
            tok.at[o, q, 1, :, at], pr.at[o, q, :, at],
            p_send.at[o, q, h], p_recv.at[o, q, h], r, mate,
        )

    def weigh(o, i, lo, hi, h):
        def tile(n, _):
            at = pl.ds(pl.multiple_of(n * d_tile, d_tile), d_tile)
            y = yr[i, lo:hi, :, at].reshape((hi - lo) * part, d_tile)
            res = lax.dot_general(
                comb[i, lo * part:hi * part], y, (((0,), (0,)), ((), ())),
                preferred_element_type=F32,
            ).astype(BF16)
            for p in range(per):
                q = order[i * per + p]
                tok[o, q, 0, :, at] = res[2 * p * count:(2 * p + 1) * count]
                tok[o, q, 1, :, at] = res[(2 * p + 1) * count:(2 * p + 2) * count]
            return 0

        lax.fori_loop(h * piece // d_tile, (h + 1) * piece // d_tile, tile, 0)
        for d in range(i * per, (i + 1) * per):
            mate_copy(o, order[d], h).start()

    def free(o, d):
        for h in range(HALVES):
            onward(o, d, h, lambda copy: copy.wait_send())
            if shared and o == OWN and d == 0:
                share(h).wait_send()
        swap(o, d).wait_send()

    def combine(i, h):
        if h == 0:
            for d in range(i * per, (i + 1) * per):
                free(OWN, d)
        for j in range(1, reach[i]):
            y_out[i, j, h].wait()
        weigh(OWN, i, 0, reach[i], h)

    def combine_partner(i):
        def work(lend):
            free(PAR, i)
            if lend:
                repaid(i).wait_recv()
            for h in range(pieces):
                weigh(PAR, i, far, rows + 1 if lend else rows, h)

        on_mid(lambda: work(i < 2))
        if i == 0:
            on_edge(lambda: work(False))
        else:
            for h in range(pieces):
                on_mid(lambda: give(i, h))

    def both_cores(o, q, h):
        at = pl.ds(h * piece, piece)
        return tok[o, q, 0, :, at].astype(F32) + pr[o, q, :, at].astype(F32)

    def given(q, i, h, col):
        at = pl.ds(h * piece, piece)
        return remote(
            tok.at[PAR, q, 0, :, at], pz.at[:, at], d_send.at[i, h], d_recv.at[1, h], r, col
        )

    def give(i, h):
        q = order[i]
        at = pl.ds(h * piece, piece)
        mate_copy(PAR, q, h).wait()
        tok[PAR, q, 0, :, at] = both_cores(PAR, q, h).astype(BF16)
        given(q, i, h, inner if i == 1 else outer).start()

    def chain(t, h, step):
        at = pl.ds(h * piece, piece)
        to = (chip + step + chips) % chips
        slot = jnp.where((to == t) & (step > 0), chips, t)
        return remote(
            tok.at[OWN, t, 0, :, at], zr.at[slot, :, at],
            z_send.at[t, h], z_recv.at[slot, h], r, 2 * to + core,
        )

    def landed(slot, h):
        at = pl.ds(h * piece, piece)
        remote(
            tok.at[OWN, chip, 0, :, at], zr.at[slot, :, at],
            z_send.at[chip, h], z_recv.at[slot, h], r, mate,
        ).wait_recv()
        return zr[slot, :, at].astype(F32)

    def reduce(k, h, step):
        at = pl.ds(h * piece, piece)
        t = jnp.where(step > 0, k, chips - 1 - k)

        @pl.when((t - chip) * step > 0)
        def _():
            mate_copy(OWN, t, h).wait()
            fed = chip != jnp.where(step > 0, 0, chips - 1)

            @pl.when(jnp.logical_not(fed))
            def _():
                tok[OWN, t, 0, :, at] = both_cores(OWN, t, h).astype(BF16)

            @pl.when(fed)
            def _():
                tok[OWN, t, 0, :, at] = (landed(t, h) + both_cores(OWN, t, h)).astype(BF16)

            chain(t, h, step).start()

    def back(h):
        at = pl.ds(h * piece, piece)
        return remote(
            tok.at[PAR, chip, 0, :, at], dr.at[:, at], d_send.at[0, h], d_recv.at[0, h], partner, c
        )

    def home_partner(h):
        at = pl.ds(h * piece, piece)
        mate_copy(PAR, chip, h).wait()
        given(chip, 1, h, inner).wait_recv()
        total = both_cores(PAR, chip, h) + pz[:, at].astype(F32)
        tok[PAR, chip, 0, :, at] = total.astype(BF16)
        back(h).start()

    def home(h):
        at = pl.ds(h * piece, piece)
        mate_copy(OWN, chip, h).wait()

        def finish(*slots_in):
            total = both_cores(OWN, chip, h)
            if shared:
                back(h).wait_recv()
                total = total + dr[:, at].astype(F32)
            for slot in slots_in:
                total = total + landed(slot, h)
            out_ref[:, at] = total.astype(BF16)

        pl.when(chip == 0)(lambda: finish(chip))
        pl.when(chip == chips - 1)(lambda: finish(chips))
        pl.when((chip > 0) & (chip < chips - 1))(lambda: finish(chip, chips))

    def run(step):
        kind = step[0]
        where = {"mid": on_mid, "end": on_edge}.get(step[-1], lambda act: act())
        if kind == "S":
            share(step[1]).start()
        elif kind == "D":
            dispatch(step[1])
        elif kind == "A":
            where(lambda: arrive(step[1], step[2]))
        elif kind == "P":
            dispatch_partner(step[1])
        elif kind == "X":
            lo, hi = (far, rows) if step[2] else (0, reach[step[1]])
            experts(step[1], lo, hi, step == ("X", 0, 0))
        elif kind == "Y":
            reply(step[1])
        elif kind == "C":
            where(lambda: [combine(step[1], h) for h in range(pieces)] and None)
        elif kind == "CP":
            combine_partner(step[1])
        elif kind == "CR":
            for h in range(pieces):
                combine(step[1], h)
                reduce(step[1], h, side)
            for h in range(pieces):
                reduce(step[1], h, -side)
        elif kind == "R":
            for way in (side, -side):
                for h in range(pieces):
                    reduce(step[1], h, way)
        else:
            ends = home_partner if step[1] else home
            where(lambda: [ends(h) for h in range(pieces)] and None)

    for step in plan(chips, per):
        with jax.named_scope("_".join(str(s) for s in step)):
            run(step)

    for o in modes:
        for d in range(1 - o, cols):
            routing(o, d, (chip + d // 2) % chips, chip).wait_send()
    for d in range(1, chips):
        for h in range(pieces):
            chain(order[d], h, side).wait_send()
    if shared:
        heard(PAR, chunks - 1)
        for i in range(2):
            on_mid(lambda: lent(i).wait_send())
            on_edge(lambda: repaid(i).wait_send())
        for h in range(pieces):
            back(h).wait_send()
            for i in (1, 2):
                on_mid(lambda: given(order[i], i, h, inner).wait_send())


def body(tokens, expert_ids, gate_probs, w_gate, w_up, w_down):
    count, choices = expert_ids.shape
    width = tokens.shape[1]
    hidden = w_gate.shape[2]
    rows = lax.axis_size("row")
    cols = lax.axis_size("col")
    slots = 5 * count * choices // (4 * rows * cols * w_gate.shape[0])
    group = 2
    while group * slots % 16:
        group *= 2
    chips = cols // 2
    chunks = chips // (group // 2)
    part = group * slots
    any_spec = pl.BlockSpec(memory_space=pl.ANY)
    dma = pltpu.SemaphoreType.DMA
    kinds = 2 if staged(chips, group // 2) else 1
    scratch = [
        pltpu.VMEM((choices, count), jnp.int32),
        pltpu.VMEM((choices, count), F32),
        pltpu.VMEM((kinds, chips, 2, 2 * choices, count), F32),
        pltpu.VMEM((kinds, chips, 2, count, width), BF16),
        pltpu.VMEM((width, hidden), BF16),
        pltpu.VMEM((width, hidden), BF16),
        pltpu.VMEM((hidden, width), BF16),
        pltpu.VMEM(((rows + 1) * part, group * count), BF16),
        pltpu.VMEM((chunks, (rows + 1) * part, group * count), BF16),
        pltpu.VMEM((rows * part, hidden), BF16),
        pltpu.VMEM((chunks, rows - 1, part, width), BF16),
        pltpu.VMEM((chunks, rows, part, width), BF16),
        pltpu.VMEM((chunks, rows + 1, part, width), BF16),
        pltpu.VMEM((kinds, chips, count, width), BF16),
        pltpu.VMEM((chips + 1, count, width), BF16),
        pltpu.VMEM((2, part, width), BF16),
        pltpu.VMEM((count, width), BF16),
        pltpu.VMEM((count, width), BF16),
        dma((6,)),
        dma((kinds, cols)), dma((kinds, chips, 2)),
        dma((HALVES,)), dma((HALVES,)),
        dma((kinds, chips + 1, HALVES)), dma((kinds, chips, HALVES)),
        dma((kinds, chips)), dma((kinds, chips)),
        dma((chunks, rows)), dma((chunks, rows)),
        dma((chunks, rows, PIECES)), dma((chunks, rows, PIECES)),
        dma((kinds, chips, PIECES)), dma((kinds, chips, PIECES)),
        dma((chips, PIECES)), dma((chips + 1, PIECES)),
        dma((2,)), dma((2,)),
        dma((2,)), dma((2,)),
        dma((3, PIECES)), dma((2, PIECES)),
    ]
    return pl.pallas_call(
        functools.partial(moe_kernel, rows, cols, slots, group, PIECES),
        out_shape=jax.ShapeDtypeStruct((count, width), BF16),
        in_specs=[any_spec] * 6,
        out_specs=pl.BlockSpec(memory_space=pltpu.VMEM),
        scratch_shapes=scratch,
        compiler_params=pltpu.CompilerParams(
            collective_id=0, has_side_effects=True, vmem_limit_bytes=67043328
        ),
    )(expert_ids.T, gate_probs.T, tokens, w_gate, w_up, w_down)


def solution(mesh):
    in_specs = (
        P(("row", "col"), None),
        P(("row", "col"), None),
        P(("row", "col"), None),
        P(("row", "col"), None, None),
        P(("row", "col"), None, None),
        P(("row", "col"), None, None),
    )
    out_specs = P(("row", "col"), None)
    return jax.shard_map(body, mesh=mesh, in_specs=in_specs, out_specs=out_specs, check_vma=False)
```

```python
import functools
import math

import jax
import jax.numpy as jnp
from jax import lax
from jax.experimental import pallas as pl
from jax.experimental.pallas import tpu as pltpu
from jax.sharding import PartitionSpec as P

MESH = pl.DeviceIdType.MESH
BF16 = jnp.bfloat16
F32 = jnp.float32
PIECES = 4
HALVES = 2
OWN, PAR = 0, 1


def flip(r, j):
    out, bit = r, 1
    while bit <= j:
        if j & bit:
            out = out + bit * (1 - 2 * ((r // bit) % 2))
        bit *= 2
    return out


def staged(chips, per):
    return per == 1 and chips == 4


def plan(chips, per):
    hops = range(1, chips)
    every = range(chips // per)
    halves = range(HALVES)
    if not staged(chips, per):
        return (
            [("A", OWN, d, h, "all") for d in hops for h in halves]
            + [("D", i, h) for i in every for h in halves]
            + [step for i in every for step in (("X", i, 0, "all"), ("Y", i))]
            + [("C", i, "all") for i in every] + [("R", k) for k in hops] + [("H", OWN, "all")]
        )
    steps = [("S", 0), ("S", 1), ("D", 0, 0), ("D", 0, 1)]
    for h in halves:
        steps += [("A", OWN, 1, h, "all"), ("A", OWN, 2, h, "mid"), ("D", 1, h)]
    steps += [("T", 0, 0), ("T", 0, 1), ("A", PAR, 0, 0, "all"), ("A", PAR, 0, 1, "all"), ("P", 0)]
    steps += [("X", 1, 0, "all"), ("Y", 1)]
    for h in halves:
        steps += [("A", OWN, 3, h, "mid"), ("A", OWN, 2, h, "end"), ("D", 2, h)]
    steps += [("L", 0), ("X", 0, 0, "all")]
    steps += [("D", 3, 0, "mid"), ("D", 3, 1, "mid"), ("CR", 1)]
    for h in halves:
        steps += [("A", OWN, 3, h, "end"), ("D", 3, h, "end")]
    return steps + [
        ("A", PAR, 1, 0, "mid"), ("A", PAR, 1, 1, "mid"), ("P", 1), ("L", 1),
        ("X", 2, 0, "all"), ("Y", 2), ("X", 1, 1, "all"),
        ("A", PAR, 2, 0, "mid"), ("A", PAR, 2, 1, "mid"), ("CP", 1), ("P", 2),
        ("X", 2, 1, "all"), ("X", 0, 1, "all"), ("X", 3, 0, "all"), ("Y", 3), ("Y", 0),
        ("CP", 2), ("CP", 0), ("CR", 2), ("H", PAR, "mid"), ("CR", 3),
        ("H", PAR, "end"), ("C", 0, "all"), ("H", OWN, "all"),
    ]


def moe_kernel(
    rows, cols, slots, group, pieces,
    ids_in, probs_in, tok_in, wg_in, wu_in, wd_in, out_hbm,
    out_ref, ids_v, probs_v, meta, tok, wg, wu, wd, disp, comb, hid, xs, xr, yr, pr, zr, es, pz, dr,
    load_sem, m_send, m_recv, pt_send, pt_recv, ztok_send, ztok_recv, ctok_send, ctok_recv,
    x_send, x_recv, y_send, y_recv, p_send, p_recv, z_send, z_recv,
    e_send, e_recv, q_send, q_recv, d_send, d_recv, out_sem,
):
    r = lax.axis_index("row")
    c = lax.axis_index("col")
    chips = cols // 2
    chip, core = c // 2, c % 2
    mate = 2 * chip + (1 - core)
    far = rows - 1
    partner = flip(r, far)
    count, width = tok_in.shape
    choices = ids_in.shape[0]
    per = group // 2
    chunks = chips // per
    part = group * slots
    shared = staged(chips, per)
    modes = (OWN, PAR) if shared else (OWN,)
    reach = [far if shared and i < chunks - 1 else rows for i in range(chunks)]
    hidden = wg.shape[1]
    f_tile = math.gcd(hidden, 256)
    d_tile = math.gcd(width // pieces, 512)
    piece = width // pieces
    half = width // HALVES

    def remote(src, dst, send, recv, row, col):
        return pltpu.make_async_remote_copy(
            src_ref=src, dst_ref=dst, send_sem=send, recv_sem=recv,
            device_id=(row, col), device_id_type=MESH,
        )

    short = jnp.minimum(chip, chips - 1 - chip)
    side = jnp.where(2 * chip < chips, 1, -1)
    inner = 2 * (chip + side) + core
    outer = 2 * ((chip - side + chips) % chips) + core
    across = 2 * ((chip + 2 * side + chips) % chips) + core
    edge = short == 0
    order, signs = [chip], [None]
    for p in range(1, chips):
        both = p <= 2 * short
        sign = jnp.where(both, side if p % 2 else -side, side)
        dist = jnp.where(both, (p + 1) // 2, p - short)
        order.append(chip + sign * dist)
        signs.append(sign)

    def on_edge(act):
        pl.when(edge)(act)

    def on_mid(act):
        pl.when(jnp.logical_not(edge))(act)

    load_tok = pltpu.make_async_copy(tok_in, tok.at[OWN, chip, 0], load_sem.at[0])
    load_ids = pltpu.make_async_copy(ids_in, ids_v, load_sem.at[1])
    load_probs = pltpu.make_async_copy(probs_in, probs_v, load_sem.at[5])
    load_w = [
        pltpu.make_async_copy(wg_in.at[0], wg, load_sem.at[2]),
        pltpu.make_async_copy(wu_in.at[0], wu, load_sem.at[3]),
        pltpu.make_async_copy(wd_in.at[0], wd, load_sem.at[4]),
    ]
    load_tok.start()
    load_ids.start()
    load_probs.start()

    barrier = pltpu.get_barrier_semaphore()
    for d in range(1, cols):
        for row in (r, partner)[:len(modes)]:
            pl.semaphore_signal(
                barrier, inc=1, device_id=(row, (c + d) % cols), device_id_type=MESH
            )
    for j in range(1, rows):
        pl.semaphore_signal(barrier, inc=1, device_id=(flip(r, j), c), device_id_type=MESH)
    load_ids.wait()
    load_probs.wait()
    meta[OWN, chip, 0, :choices] = ids_v[...].astype(F32)
    meta[OWN, chip, 0, choices:] = probs_v[...]
    pl.semaphore_wait(barrier, len(modes) * (cols - 1) + rows - 1)

    def hop(o, q, send, to, h):
        at = pl.ds(h * half, half)
        return remote(
            tok.at[o, q, 0, :, at], tok.at[o, q, 0, :, at],
            ztok_send.at[o, send, h], ztok_recv.at[o, q, h],
            r, 2 * ((to + chips) % chips) + core,
        )

    def onward(o, p, h, act):
        if o == PAR:
            if p == 0:
                act(hop(PAR, chip, 0, chip + side, h))
        elif p == 0:
            @pl.when(chip > 0)
            def _():
                act(hop(OWN, chip, 0, chip - 1, h))

            @pl.when(chip < chips - 1)
            def _():
                act(hop(OWN, chip, chips, chip + 1, h))
        else:
            to = chip - signs[p]

            @pl.when((to >= 0) & (to < chips))
            def _():
                act(hop(OWN, order[p], p, to, h))

    def swap(o, p, h):
        at = pl.ds(h * half, half)
        return remote(
            tok.at[o, order[p], 0, :, at], tok.at[o, order[p], 1, :, at],
            ctok_send.at[o, p, h], ctok_recv.at[o, p, h], r, mate,
        )

    def share(h):
        at = pl.ds(h * half, half)
        return remote(
            tok.at[OWN, chip, 0, :, at], tok.at[PAR, chip, 0, :, at],
            pt_send.at[h], pt_recv.at[h], partner, c,
        )

    def routing(o, d, t, slot):
        dist, other = d // 2, d % 2
        to = 2 * t + (core if other == 0 else 1 - core)
        return remote(
            meta.at[OWN, chip, 0], meta.at[o, slot, other],
            m_send.at[o, d], m_recv.at[o, slot, other], partner if o else r, to,
        )

    for o in modes:
        for d in range(1 - o, cols):
            routing(o, d, (chip + d // 2) % chips, chip).start()
    load_tok.wait()
    for h in range(HALVES):
        swap(OWN, 0, h).start()
        onward(OWN, 0, h, lambda copy: copy.start())
    for copy in load_w:
        copy.start()
    earlier = (
        lax.broadcasted_iota(jnp.int32, (count, count), 0)
        < lax.broadcasted_iota(jnp.int32, (count, count), 1)
    ).astype(BF16)
    slot_of = lax.broadcasted_iota(jnp.int32, (part, count), 0).astype(F32)
    lane_rows = 16
    row_id = lax.broadcasted_iota(jnp.int32, (lane_rows, count), 0)

    def route(o, i, base, experts_of):
        for s in range(group):
            q = order[i * per + s // 2]
            ids = meta[o, q, s % 2, :choices].astype(jnp.int32)
            probs = meta[o, q, s % 2, choices:]
            named = jnp.zeros((lane_rows, count), F32)
            weights = []
            for j, expert in enumerate(experts_of):
                hit = (ids == expert).astype(F32)
                named = jnp.where(row_id == j, jnp.sum(hit, axis=0, keepdims=True), named)
                weights.append(jnp.sum(hit * probs, axis=0, keepdims=True))
            rank = jnp.dot(named.astype(BF16), earlier, preferred_element_type=F32)
            key = jnp.where(named > 0.5, rank + float(s * slots), -1.0)
            for j in range(len(experts_of)):
                one = (slot_of == key[j:j + 1, :]).astype(F32)
                at = pl.ds((base + j) * part, part)
                disp[at, s * count:(s + 1) * count] = one.astype(BF16)
                comb[i, at, s * count:(s + 1) * count] = (one * weights[j]).astype(BF16)

    y_out = {}

    def arrive(o, d, h):
        if o == PAR and d == 0:
            share(h).wait_recv()
        else:
            hop(o, order[d], d, chip, h).wait_recv()
        onward(o, d, h, lambda copy: copy.start())
        swap(o, d, h).start()

    def heard(o, i):
        for d in range(i * per, (i + 1) * per):
            for other in range(1 if o == OWN and d == 0 else 0, 2):
                routing(o, other, order[d], order[d]).wait_recv()

    def blocks(o, i, at):
        return jnp.concatenate(
            [tok[o, q, :, :, at].reshape(2 * count, d_tile) for q in order[i * per:(i + 1) * per]]
        )

    def dispatch(i, h):
        if h == 0:
            heard(OWN, i)
            route(OWN, i, 0, [flip(r, j) * cols + c for j in range(reach[i])])
        for d in range(i * per, (i + 1) * per):
            swap(OWN, d, h).wait_recv()
        near = reach[i] * part

        def tile(n, _):
            at = pl.ds(pl.multiple_of(n * d_tile, d_tile), d_tile)
            res = jnp.dot(disp[:near], blocks(OWN, i, at), preferred_element_type=F32).astype(BF16)
            xr[i, 0, :, at] = res[:part]
            xs[i, :reach[i] - 1, :, at] = res[part:].reshape(reach[i] - 1, part, d_tile)
            return 0

        lax.fori_loop(h * half // d_tile, (h + 1) * half // d_tile, tile, 0)

    def slot_copy(i, j, h):
        at = pl.ds(h * half, half)
        return remote(
            xs.at[i, j - 1, :, at], xr.at[i, j, :, at],
            x_send.at[i, j, h], x_recv.at[i, j, h], flip(r, j), c,
        )

    def transmit(i, h):
        for j in range(1, reach[i]):
            slot_copy(i, j, h).start()

    def lent(i):
        return remote(es.at[i], xr.at[i + 1, far], e_send.at[i], e_recv.at[i], r, outer)

    def repaid(i):
        return remote(
            yr.at[i + 1, far], yr.at[0, rows + i], q_send.at[i], q_recv.at[i],
            r, across if i else inner,
        )

    def dispatch_partner(i):
        def work(lend):
            heard(PAR, i)
            mine = [r * cols + c] + ([r * cols + outer] if lend else [])
            route(PAR, i, far, mine + ([r * cols + across] if lend and i == 0 else []))
            for h in range(HALVES):
                swap(PAR, i, h).wait_recv()

            def tile(n, _):
                at = pl.ds(pl.multiple_of(n * d_tile, d_tile), d_tile)
                res = jnp.dot(
                    disp[far * part:(far + len(mine)) * part], blocks(PAR, i, at),
                    preferred_element_type=F32,
                ).astype(BF16)
                xr[i, far, :, at] = res[:part]
                if lend:
                    es[i, :, at] = res[part:]
                return 0

            lax.fori_loop(0, width // d_tile, tile, 0)

        on_mid(lambda: work(i < 2))
        on_edge(lambda: heard(PAR, i) if i else work(False))

    def experts(i, lo, hi, first):
        if lo == 0:
            for j in range(1, hi):
                for h in range(HALVES):
                    slot_copy(i, j, h).wait()
        elif i:
            on_edge(lambda: lent(i - 1).wait_recv())
        if first:
            for copy in load_w:
                copy.wait()
        size = (hi - lo) * part

        def up_tile(n, _):
            at = pl.ds(pl.multiple_of(n * f_tile, f_tile), f_tile)
            x = xr[i, lo:hi].reshape(size, width)
            gate = jnp.dot(x, wg[:, at], preferred_element_type=F32)
            up = jnp.dot(x, wu[:, at], preferred_element_type=F32)
            hid[:size, at] = (gate / (1.0 + jnp.exp(-gate)) * up).astype(BF16)
            return 0

        lax.fori_loop(0, hidden // f_tile, up_tile, 0)

        def down_tile(n, _):
            at = pl.ds(pl.multiple_of(n * d_tile, d_tile), d_tile)
            res = jnp.dot(hid[:size], wd[:, at], preferred_element_type=F32).astype(BF16)
            if lo == 0:
                yr[i, 0, :, at] = res[:part]
                xs[i, :hi - 1, :, at] = res[part:].reshape(hi - 1, part, d_tile)
            else:
                yr[i, far, :, at] = res
            return 0

        lax.fori_loop(0, width // d_tile, down_tile, 0)
        if lo and i:
            on_edge(lambda: repaid(i - 1).start())

    def reply(i):
        for h in range(pieces):
            at = pl.ds(h * piece, piece)
            for j in range(1, reach[i]):
                copy = remote(
                    xs.at[i, j - 1, :, at], yr.at[i, j, :, at],
                    y_send.at[i, j, h], y_recv.at[i, j, h], flip(r, j), c,
                )
                copy.start()
                y_out[i, j, h] = copy

    def mate_copy(o, q, h):
        at = pl.ds(h * piece, piece)
        return remote(
            tok.at[o, q, 1, :, at], pr.at[o, q, :, at],
            p_send.at[o, q, h], p_recv.at[o, q, h], r, mate,
        )

    def weigh(o, i, lo, hi, h):
        def tile(n, _):
            at = pl.ds(pl.multiple_of(n * d_tile, d_tile), d_tile)
            y = yr[i, lo:hi, :, at].reshape((hi - lo) * part, d_tile)
            res = lax.dot_general(
                comb[i, lo * part:hi * part], y, (((0,), (0,)), ((), ())),
                preferred_element_type=F32,
            ).astype(BF16)
            for p in range(per):
                q = order[i * per + p]
                tok[o, q, 0, :, at] = res[2 * p * count:(2 * p + 1) * count]
                tok[o, q, 1, :, at] = res[(2 * p + 1) * count:(2 * p + 2) * count]
            return 0

        lax.fori_loop(h * piece // d_tile, (h + 1) * piece // d_tile, tile, 0)
        for d in range(i * per, (i + 1) * per):
            mate_copy(o, order[d], h).start()

    def free(o, d):
        for h in range(HALVES):
            onward(o, d, h, lambda copy: copy.wait_send())
            if shared and o == OWN and d == 0:
                share(h).wait_send()
            swap(o, d, h).wait_send()

    def combine(i, h):
        if h == 0:
            for d in range(i * per, (i + 1) * per):
                free(OWN, d)
        for j in range(1, reach[i]):
            y_out[i, j, h].wait()
        weigh(OWN, i, 0, reach[i], h)

    def combine_partner(i):
        def work(lent_out):
            free(PAR, i)
            for j in range(lent_out):
                repaid(j).wait_recv()
            for h in range(pieces):
                weigh(PAR, i, far, rows + lent_out, h)

        on_mid(lambda: work(0 if i else 2))
        if i == 0:
            on_edge(lambda: work(0))
        else:
            for h in range(pieces):
                on_mid(lambda: give(i, h))

    def both_cores(o, q, h):
        at = pl.ds(h * piece, piece)
        return tok[o, q, 0, :, at].astype(F32) + pr[o, q, :, at].astype(F32)

    def given(q, i, h, col):
        at = pl.ds(h * piece, piece)
        return remote(
            tok.at[PAR, q, 0, :, at], pz.at[:, at], d_send.at[i, h], d_recv.at[1, h], r, col
        )

    def give(i, h):
        q = order[i]
        at = pl.ds(h * piece, piece)
        mate_copy(PAR, q, h).wait()
        tok[PAR, q, 0, :, at] = both_cores(PAR, q, h).astype(BF16)
        given(q, i, h, inner if i == 1 else outer).start()

    def chain(t, h, step):
        at = pl.ds(h * piece, piece)
        to = (chip + step + chips) % chips
        slot = jnp.where((to == t) & (step > 0), chips, t)
        return remote(
            tok.at[OWN, t, 0, :, at], zr.at[slot, :, at],
            z_send.at[t, h], z_recv.at[slot, h], r, 2 * to + core,
        )

    def landed(slot, h):
        at = pl.ds(h * piece, piece)
        remote(
            tok.at[OWN, chip, 0, :, at], zr.at[slot, :, at],
            z_send.at[chip, h], z_recv.at[slot, h], r, mate,
        ).wait_recv()
        return zr[slot, :, at].astype(F32)

    def reduce(k, h, step):
        at = pl.ds(h * piece, piece)
        t = jnp.where(step > 0, k, chips - 1 - k)

        @pl.when((t - chip) * step > 0)
        def _():
            mate_copy(OWN, t, h).wait()
            fed = chip != jnp.where(step > 0, 0, chips - 1)

            @pl.when(jnp.logical_not(fed))
            def _():
                tok[OWN, t, 0, :, at] = both_cores(OWN, t, h).astype(BF16)

            @pl.when(fed)
            def _():
                tok[OWN, t, 0, :, at] = (landed(t, h) + both_cores(OWN, t, h)).astype(BF16)

            chain(t, h, step).start()

    def back(h):
        at = pl.ds(h * piece, piece)
        return remote(
            tok.at[PAR, chip, 0, :, at], dr.at[:, at], d_send.at[0, h], d_recv.at[0, h], partner, c
        )

    def home_partner(h):
        at = pl.ds(h * piece, piece)
        mate_copy(PAR, chip, h).wait()
        given(chip, 1, h, inner).wait_recv()
        total = both_cores(PAR, chip, h) + pz[:, at].astype(F32)
        tok[PAR, chip, 0, :, at] = total.astype(BF16)
        back(h).start()

    def leave(h):
        at = pl.ds(h * piece, piece)
        return pltpu.make_async_copy(out_ref.at[:, at], out_hbm.at[:, at], out_sem.at[h])

    def home(h):
        at = pl.ds(h * piece, piece)
        mate_copy(OWN, chip, h).wait()

        def finish(*slots_in):
            total = both_cores(OWN, chip, h)
            if shared:
                back(h).wait_recv()
                total = total + dr[:, at].astype(F32)
            for slot in slots_in:
                total = total + landed(slot, h)
            out_ref[:, at] = total.astype(BF16)

        pl.when(chip == 0)(lambda: finish(chip))
        pl.when(chip == chips - 1)(lambda: finish(chips))
        pl.when((chip > 0) & (chip < chips - 1))(lambda: finish(chip, chips))
        leave(h).start()

    def run(step):
        kind = step[0]
        where = {"mid": on_mid, "end": on_edge}.get(step[-1], lambda act: act())
        if kind == "S":
            share(step[1]).start()
        elif kind == "D":
            def both():
                dispatch(step[1], step[2])
                if step[1] or not shared:
                    transmit(step[1], step[2])

            where(both)
        elif kind == "T":
            transmit(step[1], step[2])
        elif kind == "L":
            on_mid(lambda: lent(step[1]).start())
        elif kind == "A":
            where(lambda: arrive(step[1], step[2], step[3]))
        elif kind == "P":
            dispatch_partner(step[1])
        elif kind == "X":
            lo, hi = (far, rows) if step[2] else (0, reach[step[1]])
            where(lambda: experts(step[1], lo, hi, step == first))
        elif kind == "Y":
            reply(step[1])
        elif kind == "C":
            where(lambda: [combine(step[1], h) for h in range(pieces)] and None)
        elif kind == "CP":
            combine_partner(step[1])
        elif kind == "CR":
            for h in range(pieces):
                combine(step[1], h)
                reduce(step[1], h, side)
            for h in range(pieces):
                reduce(step[1], h, -side)
        elif kind == "R":
            for way in (side, -side):
                for h in range(pieces):
                    reduce(step[1], h, way)
        else:
            ends = home_partner if step[1] else home
            where(lambda: [ends(h) for h in range(pieces)] and None)

    steps = plan(chips, per)
    first = next(step for step in steps if step[0] == "X")
    for step in steps:
        with jax.named_scope("_".join(str(s) for s in step)):
            run(step)

    with jax.named_scope("settle"):
        for o in modes:
            for d in range(1 - o, cols):
                routing(o, d, (chip + d // 2) % chips, chip).wait_send()
        for h in range(pieces):
            for d in range(1, chips):
                chain(order[d], h, side).wait_send()
            leave(h).wait()
        if shared:
            heard(PAR, chunks - 1)
            for i in range(2):
                on_mid(lambda: lent(i).wait_send())
                on_edge(lambda: repaid(i).wait_send())
            for h in range(pieces):
                back(h).wait_send()
                for i in (1, 2):
                    on_mid(lambda: given(order[i], i, h, inner).wait_send())


def body(tokens, expert_ids, gate_probs, w_gate, w_up, w_down):
    count, choices = expert_ids.shape
    width = tokens.shape[1]
    hidden = w_gate.shape[2]
    rows = lax.axis_size("row")
    cols = lax.axis_size("col")
    slots = 5 * count * choices // (4 * rows * cols * w_gate.shape[0])
    group = 2
    while group * slots % 16:
        group *= 2
    chips = cols // 2
    chunks = chips // (group // 2)
    part = group * slots
    any_spec = pl.BlockSpec(memory_space=pl.ANY)
    dma = pltpu.SemaphoreType.DMA
    kinds = 2 if staged(chips, group // 2) else 1
    scratch = [
        pltpu.VMEM((count, width), BF16),
        pltpu.VMEM((choices, count), jnp.int32),
        pltpu.VMEM((choices, count), F32),
        pltpu.VMEM((kinds, chips, 2, 2 * choices, count), F32),
        pltpu.VMEM((kinds, chips, 2, count, width), BF16),
        pltpu.VMEM((width, hidden), BF16),
        pltpu.VMEM((width, hidden), BF16),
        pltpu.VMEM((hidden, width), BF16),
        pltpu.VMEM(((rows + 2) * part, group * count), BF16),
        pltpu.VMEM((chunks, (rows + 2) * part, group * count), BF16),
        pltpu.VMEM((rows * part, hidden), BF16),
        pltpu.VMEM((chunks, rows - 1, part, width), BF16),
        pltpu.VMEM((chunks, rows, part, width), BF16),
        pltpu.VMEM((chunks, rows + 2, part, width), BF16),
        pltpu.VMEM((kinds, chips, count, width), BF16),
        pltpu.VMEM((chips + 1, count, width), BF16),
        pltpu.VMEM((2, part, width), BF16),
        pltpu.VMEM((count, width), BF16),
        pltpu.VMEM((count, width), BF16),
        dma((6,)),
        dma((kinds, cols)), dma((kinds, chips, 2)),
        dma((HALVES,)), dma((HALVES,)),
        dma((kinds, chips + 1, HALVES)), dma((kinds, chips, HALVES)),
        dma((kinds, chips, HALVES)), dma((kinds, chips, HALVES)),
        dma((chunks, rows, HALVES)), dma((chunks, rows, HALVES)),
        dma((chunks, rows, PIECES)), dma((chunks, rows, PIECES)),
        dma((kinds, chips, PIECES)), dma((kinds, chips, PIECES)),
        dma((chips, PIECES)), dma((chips + 1, PIECES)),
        dma((2,)), dma((2,)),
        dma((2,)), dma((2,)),
        dma((3, PIECES)), dma((2, PIECES)), dma((PIECES,)),
    ]
    return pl.pallas_call(
        functools.partial(moe_kernel, rows, cols, slots, group, PIECES),
        out_shape=jax.ShapeDtypeStruct((count, width), BF16),
        in_specs=[any_spec] * 6,
        out_specs=pl.BlockSpec(memory_space=pl.ANY),
        scratch_shapes=scratch,
        compiler_params=pltpu.CompilerParams(
            collective_id=0, has_side_effects=True, vmem_limit_bytes=67043328
        ),
    )(expert_ids.T, gate_probs.T, tokens, w_gate, w_up, w_down)


def solution(mesh):
    in_specs = (
        P(("row", "col"), None),
        P(("row", "col"), None),
        P(("row", "col"), None),
        P(("row", "col"), None, None),
        P(("row", "col"), None, None),
        P(("row", "col"), None, None),
    )
    out_specs = P(("row", "col"), None)
    return jax.shard_map(body, mesh=mesh, in_specs=in_specs, out_specs=out_specs, check_vma=False)
```

```python
import functools
import math

import jax
import jax.numpy as jnp
from jax import lax
from jax.experimental import pallas as pl
from jax.experimental.pallas import tpu as pltpu
from jax.sharding import PartitionSpec as P

MESH = pl.DeviceIdType.MESH
BF16 = jnp.bfloat16
F32 = jnp.float32
PIECES = 4
HALVES = 2
OWN, PAR = 0, 1


def flip(r, j):
    out, bit = r, 1
    while bit <= j:
        if j & bit:
            out = out + bit * (1 - 2 * ((r // bit) % 2))
        bit *= 2
    return out


def staged(chips, per):
    return per == 1 and chips == 4


def plan(chips, per):
    hops = range(1, chips)
    every = range(chips // per)
    halves = range(HALVES)
    if not staged(chips, per):
        return (
            [("A", OWN, d, h, "all") for d in hops for h in halves]
            + [("D", i, h) for i in every for h in halves]
            + [step for i in every for step in (("X", i, 0, "all"), ("Y", i))]
            + [("C", i, "all") for i in every] + [("R", k) for k in hops] + [("H", OWN, "all")]
        )
    steps = [("S",), ("D", 0, 0), ("D", 0, 1)]
    for h in halves:
        steps += [("A", OWN, 1, h, "all"), ("A", OWN, 2, h, "mid"), ("D", 1, h)]
    steps += [("T", 0, 0), ("T", 0, 1), ("A", PAR, 0, 0, "all"), ("P", 0)]
    steps += [("X", 1, 0, "all"), ("Y", 1)]
    for h in halves:
        steps += [("A", OWN, 3, h, "mid"), ("A", OWN, 2, h, "end"), ("D", 2, h)]
    steps += [("L", 0), ("X", 0, 0, "all")]
    steps += [("D", 3, 0, "mid"), ("D", 3, 1, "mid"), ("CR", 1)]
    for h in halves:
        steps += [("A", OWN, 3, h, "end"), ("D", 3, h, "end")]
    return steps + [
        ("A", PAR, 1, 0, "mid"), ("P", 1), ("L", 1),
        ("X", 2, 0, "all"), ("Y", 2), ("X", 1, 1, "all"),
        ("A", PAR, 2, 0, "mid"), ("CP", 1), ("P", 2),
        ("X", 2, 1, "all"), ("X", 0, 1, "all"), ("X", 3, 0, "all"), ("Y", 3), ("Y", 0),
        ("CP", 2), ("CP", 0), ("CR", 2), ("H", PAR, "mid"), ("CR", 3),
        ("H", PAR, "end"), ("C", 0, "all"), ("H", OWN, "all"),
    ]


def moe_kernel(
    rows, cols, slots, group, pieces,
    ids_in, probs_in, tok_in, wg_in, wu_in, wd_in, out_hbm,
    out_ref, ids_v, probs_v, meta, tok, wg, wu, wd, disp, comb, hid, xs, xr, yr, pr, zr, es, pz, dr,
    load_sem, m_send, m_recv, pt_send, pt_recv, ztok_send, ztok_recv, gtok_send, gtok_recv,
    ctok_send, ctok_recv, stok_recv, x_send, x_recv, y_send, y_recv, p_send, p_recv, g_recv,
    z_send, z_recv, e_send, e_recv, q_send, q_recv, d_send, d_recv, pz_recv, out_sem,
):
    r = lax.axis_index("row")
    c = lax.axis_index("col")
    chips = cols // 2
    chip, core = c // 2, c % 2
    mate = 2 * chip + (1 - core)
    far = rows - 1
    partner = flip(r, far)
    count, width = tok_in.shape
    choices = ids_in.shape[0]
    per = group // 2
    chunks = chips // per
    part = group * slots
    shared = staged(chips, per)
    modes = (OWN, PAR) if shared else (OWN,)
    reach = [far if shared and i < chunks - 1 else rows for i in range(chunks)]
    hidden = wg.shape[1]
    f_tile = math.gcd(hidden, 256)
    d_tile = math.gcd(width // pieces, 512)
    piece = width // pieces
    half = width // HALVES

    def remote(src, dst, send, recv, row, col):
        return pltpu.make_async_remote_copy(
            src_ref=src, dst_ref=dst, send_sem=send, recv_sem=recv,
            device_id=(row, col), device_id_type=MESH,
        )

    def taken(ref, sem):
        pltpu.make_async_copy(ref, ref, sem).wait()

    short = jnp.minimum(chip, chips - 1 - chip)
    side = jnp.where(2 * chip < chips, 1, -1)
    inner = 2 * (chip + side) + core
    outer = 2 * ((chip - side + chips) % chips) + core
    across = 2 * ((chip + 2 * side + chips) % chips) + core
    edge = short == 0
    order, signs = [chip], [None]
    for p in range(1, chips):
        both = p <= 2 * short
        sign = jnp.where(both, side if p % 2 else -side, side)
        dist = jnp.where(both, (p + 1) // 2, p - short)
        order.append(chip + sign * dist)
        signs.append(sign)

    def on_edge(act):
        pl.when(edge)(act)

    def on_mid(act):
        pl.when(jnp.logical_not(edge))(act)

    load_tok = pltpu.make_async_copy(tok_in, tok.at[OWN, chip, 0], load_sem.at[0])
    load_ids = pltpu.make_async_copy(ids_in, ids_v, load_sem.at[1])
    load_probs = pltpu.make_async_copy(probs_in, probs_v, load_sem.at[5])
    load_w = [
        pltpu.make_async_copy(wg_in.at[0], wg, load_sem.at[2]),
        pltpu.make_async_copy(wu_in.at[0], wu, load_sem.at[3]),
        pltpu.make_async_copy(wd_in.at[0], wd, load_sem.at[4]),
    ]
    load_tok.start()
    load_ids.start()
    load_probs.start()

    barrier = pltpu.get_barrier_semaphore()
    for d in range(1, cols):
        for row in (r, partner)[:len(modes)]:
            pl.semaphore_signal(
                barrier, inc=1, device_id=(row, (c + d) % cols), device_id_type=MESH
            )
    for j in range(1, rows):
        pl.semaphore_signal(barrier, inc=1, device_id=(flip(r, j), c), device_id_type=MESH)
    load_ids.wait()
    load_probs.wait()
    meta[OWN, chip, 0, :choices] = ids_v[...].astype(F32)
    meta[OWN, chip, 0, choices:] = probs_v[...]
    pl.semaphore_wait(barrier, len(modes) * (cols - 1) + rows - 1)

    def hop(o, q, send, to, h):
        at = pl.ds(h * half, half) if o == OWN else pl.ds(0, width)
        return remote(
            tok.at[o, q, 0, :, at], tok.at[o, q, 0, :, at],
            ztok_send.at[send] if o == OWN else gtok_send.at[0],
            ztok_recv.at[q, h] if o == OWN else gtok_recv.at[q],
            r, 2 * ((to + chips) % chips) + core,
        )

    def sent(o, p):
        q = order[p]
        if o == PAR:
            if p == 0:
                taken(tok.at[PAR, q, 0], gtok_send.at[0])
        elif p == 0:
            pl.when(chip > 0)(lambda: taken(tok.at[OWN, q, 0], ztok_send.at[0]))
            pl.when(chip < chips - 1)(lambda: taken(tok.at[OWN, q, 0], ztok_send.at[chips]))
        else:
            to = chip - signs[p]
            pl.when((to >= 0) & (to < chips))(
                lambda: taken(tok.at[OWN, q, 0], ztok_send.at[p])
            )

    def onward(o, p, h, act):
        if o == PAR:
            if p == 0:
                act(hop(PAR, chip, 0, chip + side, h))
        elif p == 0:
            @pl.when(chip > 0)
            def _():
                act(hop(OWN, chip, 0, chip - 1, h))

            @pl.when(chip < chips - 1)
            def _():
                act(hop(OWN, chip, chips, chip + 1, h))
        else:
            to = chip - signs[p]

            @pl.when((to >= 0) & (to < chips))
            def _():
                act(hop(OWN, order[p], p, to, h))

    def swap(o, p, h):
        at = pl.ds(h * half, half) if o == OWN else pl.ds(0, width)
        return remote(
            tok.at[o, order[p], 0, :, at], tok.at[o, order[p], 1, :, at],
            ctok_send.at[o, p], ctok_recv.at[p, h] if o == OWN else stok_recv.at[p], r, mate,
        )

    def share():
        return remote(
            tok.at[OWN, chip, 0], tok.at[PAR, chip, 0], pt_send.at[0], pt_recv.at[0], partner, c
        )

    def routing(o, d, t, slot):
        dist, other = d // 2, d % 2
        to = 2 * t + (core if other == 0 else 1 - core)
        return remote(
            meta.at[OWN, chip, 0], meta.at[o, slot, other],
            m_send.at[2 if o else min(dist, 1)], m_recv.at[o, slot], partner if o else r, to,
        )

    for o in modes:
        for d in range(1 - o, cols):
            routing(o, d, (chip + d // 2) % chips, chip).start()
    load_tok.wait()
    for h in range(HALVES):
        swap(OWN, 0, h).start()
        onward(OWN, 0, h, lambda copy: copy.start())
    for copy in load_w:
        copy.start()
    earlier = (
        lax.broadcasted_iota(jnp.int32, (count, count), 0)
        < lax.broadcasted_iota(jnp.int32, (count, count), 1)
    ).astype(BF16)
    slot_of = lax.broadcasted_iota(jnp.int32, (part, count), 0).astype(F32)
    lane_rows = 16
    row_id = lax.broadcasted_iota(jnp.int32, (lane_rows, count), 0)

    def route(o, i, base, experts_of):
        for s in range(group):
            q = order[i * per + s // 2]
            ids = meta[o, q, s % 2, :choices].astype(jnp.int32)
            probs = meta[o, q, s % 2, choices:]
            named = jnp.zeros((lane_rows, count), F32)
            weights = []
            for j, expert in enumerate(experts_of):
                hit = (ids == expert).astype(F32)
                named = jnp.where(row_id == j, jnp.sum(hit, axis=0, keepdims=True), named)
                weights.append(jnp.sum(hit * probs, axis=0, keepdims=True))
            rank = jnp.dot(named.astype(BF16), earlier, preferred_element_type=F32)
            key = jnp.where(named > 0.5, rank + float(s * slots), -1.0)
            for j in range(len(experts_of)):
                one = (slot_of == key[j:j + 1, :]).astype(F32)
                at = pl.ds((base + j) * part, part)
                disp[at, s * count:(s + 1) * count] = one.astype(BF16)
                comb[i, at, s * count:(s + 1) * count] = (one * weights[j]).astype(BF16)


    def arrive(o, d, h):
        if o == PAR and d == 0:
            share().wait_recv()
        else:
            hop(o, order[d], d, chip, h).wait_recv()
        onward(o, d, h, lambda copy: copy.start())
        swap(o, d, h).start()

    def heard(o, i):
        for d in range(i * per, (i + 1) * per):
            home_only = o == OWN and d == 0
            taken(
                meta.at[o, order[d], 1] if home_only else meta.at[o, order[d]],
                m_recv.at[o, order[d]],
            )

    def blocks(o, i, at):
        return jnp.concatenate(
            [tok[o, q, :, :, at].reshape(2 * count, d_tile) for q in order[i * per:(i + 1) * per]]
        )

    def dispatch(i, h):
        if h == 0:
            heard(OWN, i)
            route(OWN, i, 0, [flip(r, j) * cols + c for j in range(reach[i])])
        for d in range(i * per, (i + 1) * per):
            swap(OWN, d, h).wait_recv()
        near = reach[i] * part

        def tile(n, _):
            at = pl.ds(pl.multiple_of(n * d_tile, d_tile), d_tile)
            res = jnp.dot(disp[:near], blocks(OWN, i, at), preferred_element_type=F32).astype(BF16)
            xr[i, 0, :, at] = res[:part]
            xs[i, :reach[i] - 1, :, at] = res[part:].reshape(reach[i] - 1, part, d_tile)
            return 0

        lax.fori_loop(h * half // d_tile, (h + 1) * half // d_tile, tile, 0)

    def slot_copy(i, j, h):
        at = pl.ds(h * half, half)
        return remote(
            xs.at[i, j - 1, :, at], xr.at[i, j, :, at],
            x_send.at[i], x_recv.at[i], flip(r, j), c,
        )

    def transmit(i, h):
        for j in range(1, reach[i]):
            slot_copy(i, j, h).start()

    def lent(i):
        return remote(es.at[i], xr.at[i + 1, far], e_send.at[i], e_recv.at[i], r, outer)

    def repaid(i):
        return remote(
            yr.at[i + 1, far], yr.at[0, rows + i], q_send.at[i], q_recv.at[i],
            r, across if i else inner,
        )

    def dispatch_partner(i):
        def work(lend):
            heard(PAR, i)
            mine = [r * cols + c] + ([r * cols + outer] if lend else [])
            route(PAR, i, far, mine + ([r * cols + across] if lend and i == 0 else []))
            swap(PAR, i, 0).wait_recv()

            def tile(n, _):
                at = pl.ds(pl.multiple_of(n * d_tile, d_tile), d_tile)
                res = jnp.dot(
                    disp[far * part:(far + len(mine)) * part], blocks(PAR, i, at),
                    preferred_element_type=F32,
                ).astype(BF16)
                xr[i, far, :, at] = res[:part]
                if lend:
                    es[i, :, at] = res[part:]
                return 0

            lax.fori_loop(0, width // d_tile, tile, 0)

        on_mid(lambda: work(i < 2))
        on_edge(lambda: heard(PAR, i) if i else work(False))

    def experts(i, lo, hi, first):
        if lo == 0:
            taken(xs.at[i, :hi - 1], x_send.at[i])
            taken(xr.at[i, 1:hi], x_recv.at[i])
        elif i:
            on_edge(lambda: lent(i - 1).wait_recv())
        if first:
            for copy in load_w:
                copy.wait()
        size = (hi - lo) * part

        def up_tile(n, _):
            at = pl.ds(pl.multiple_of(n * f_tile, f_tile), f_tile)
            x = xr[i, lo:hi].reshape(size, width)
            gate = jnp.dot(x, wg[:, at], preferred_element_type=F32)
            up = jnp.dot(x, wu[:, at], preferred_element_type=F32)
            hid[:size, at] = (gate / (1.0 + jnp.exp(-gate)) * up).astype(BF16)
            return 0

        lax.fori_loop(0, hidden // f_tile, up_tile, 0)

        def down_tile(n, _):
            at = pl.ds(pl.multiple_of(n * d_tile, d_tile), d_tile)
            res = jnp.dot(hid[:size], wd[:, at], preferred_element_type=F32).astype(BF16)
            if lo == 0:
                yr[i, 0, :, at] = res[:part]
                xs[i, :hi - 1, :, at] = res[part:].reshape(hi - 1, part, d_tile)
            else:
                yr[i, far, :, at] = res
            return 0

        lax.fori_loop(0, width // d_tile, down_tile, 0)
        if lo and i:
            on_edge(lambda: repaid(i - 1).start())

    def reply(i):
        for h in range(pieces):
            at = pl.ds(h * piece, piece)
            for j in range(1, reach[i]):
                remote(
                    xs.at[i, j - 1, :, at], yr.at[i, j, :, at],
                    y_send.at[i], y_recv.at[i, h], flip(r, j), c,
                ).start()

    def mate_copy(o, q, h):
        at = pl.ds(h * piece, piece)
        return remote(
            tok.at[o, q, 1, :, at], pr.at[o, q, :, at],
            p_send.at[q if o else chips], p_recv.at[q, h] if o == OWN else g_recv.at[q], r, mate,
        )

    def weigh(o, i, lo, hi, h):
        def tile(n, _):
            at = pl.ds(pl.multiple_of(n * d_tile, d_tile), d_tile)
            y = yr[i, lo:hi, :, at].reshape((hi - lo) * part, d_tile)
            res = lax.dot_general(
                comb[i, lo * part:hi * part], y, (((0,), (0,)), ((), ())),
                preferred_element_type=F32,
            ).astype(BF16)
            for p in range(per):
                q = order[i * per + p]
                tok[o, q, 0, :, at] = res[2 * p * count:(2 * p + 1) * count]
                tok[o, q, 1, :, at] = res[(2 * p + 1) * count:(2 * p + 2) * count]
            return 0

        lax.fori_loop(h * piece // d_tile, (h + 1) * piece // d_tile, tile, 0)
        for d in range(i * per, (i + 1) * per):
            mate_copy(o, order[d], h).start()

    def free(o, d):
        sent(o, d)
        if shared and o == OWN and d == 0:
            share().wait_send()
        taken(tok.at[o, order[d], 0], ctok_send.at[o, d])

    def combine(i, h):
        if h == 0:
            for d in range(i * per, (i + 1) * per):
                free(OWN, d)
        taken(yr.at[i, 1:reach[i], :, pl.ds(h * piece, piece)], y_recv.at[i, h])
        weigh(OWN, i, 0, reach[i], h)

    def combine_partner(i):
        def work(lent_out):
            free(PAR, i)
            for j in range(lent_out):
                repaid(j).wait_recv()
            for h in range(pieces):
                weigh(PAR, i, far, rows + lent_out, h)

        on_mid(lambda: work(0 if i else 2))
        if i == 0:
            on_edge(lambda: work(0))
        else:
            on_mid(lambda: give(i))

    def both_cores(o, q, h):
        at = pl.ds(h * piece, piece)
        return tok[o, q, 0, :, at].astype(F32) + pr[o, q, :, at].astype(F32)

    def given(q, i, h, col):
        at = pl.ds(h * piece, piece)
        return remote(
            tok.at[PAR, q, 0, :, at], pz.at[:, at], d_send.at[i], pz_recv.at[0], r, col
        )

    def give(i):
        q = order[i]
        taken(pr.at[PAR, q], g_recv.at[q])
        for h in range(pieces):
            at = pl.ds(h * piece, piece)
            tok[PAR, q, 0, :, at] = both_cores(PAR, q, h).astype(BF16)
            given(q, i, h, inner if i == 1 else outer).start()

    def chain(t, h, step):
        at = pl.ds(h * piece, piece)
        to = (chip + step + chips) % chips
        slot = jnp.where((to == t) & (step > 0), chips, t)
        return remote(
            tok.at[OWN, t, 0, :, at], zr.at[slot, :, at],
            z_send.at[0], z_recv.at[slot, h], r, 2 * to + core,
        )

    def landed(slot, h):
        at = pl.ds(h * piece, piece)
        remote(
            tok.at[OWN, chip, 0, :, at], zr.at[slot, :, at],
            z_send.at[0], z_recv.at[slot, h], r, mate,
        ).wait_recv()
        return zr[slot, :, at].astype(F32)

    def reduce(k, h, step):
        at = pl.ds(h * piece, piece)
        t = jnp.where(step > 0, k, chips - 1 - k)

        @pl.when((t - chip) * step > 0)
        def _():
            mate_copy(OWN, t, h).wait_recv()
            fed = chip != jnp.where(step > 0, 0, chips - 1)

            @pl.when(jnp.logical_not(fed))
            def _():
                tok[OWN, t, 0, :, at] = both_cores(OWN, t, h).astype(BF16)

            @pl.when(fed)
            def _():
                tok[OWN, t, 0, :, at] = (landed(t, h) + both_cores(OWN, t, h)).astype(BF16)

            chain(t, h, step).start()

    def back(h):
        at = pl.ds(h * piece, piece)
        return remote(
            tok.at[PAR, chip, 0, :, at], dr.at[:, at], d_send.at[0], d_recv.at[h], partner, c
        )

    def home_partner(h):
        at = pl.ds(h * piece, piece)
        if h == 0:
            taken(pr.at[PAR, chip], g_recv.at[chip])
            taken(pz, pz_recv.at[0])
        total = both_cores(PAR, chip, h) + pz[:, at].astype(F32)
        tok[PAR, chip, 0, :, at] = total.astype(BF16)
        back(h).start()

    def leave(h):
        at = pl.ds(h * piece, piece)
        return pltpu.make_async_copy(out_ref.at[:, at], out_hbm.at[:, at], out_sem.at[0])

    def home(h):
        at = pl.ds(h * piece, piece)
        mate_copy(OWN, chip, h).wait_recv()

        def finish(*slots_in):
            total = both_cores(OWN, chip, h)
            if shared:
                back(h).wait_recv()
                total = total + dr[:, at].astype(F32)
            for slot in slots_in:
                total = total + landed(slot, h)
            out_ref[:, at] = total.astype(BF16)

        pl.when(chip == 0)(lambda: finish(chip))
        pl.when(chip == chips - 1)(lambda: finish(chips))
        pl.when((chip > 0) & (chip < chips - 1))(lambda: finish(chip, chips))
        leave(h).start()

    def run(step):
        kind = step[0]
        where = {"mid": on_mid, "end": on_edge}.get(step[-1], lambda act: act())
        if kind == "S":
            share().start()
        elif kind == "D":
            def both():
                dispatch(step[1], step[2])
                if step[1] or not shared:
                    transmit(step[1], step[2])

            where(both)
        elif kind == "T":
            transmit(step[1], step[2])
        elif kind == "L":
            on_mid(lambda: lent(step[1]).start())
        elif kind == "A":
            where(lambda: arrive(step[1], step[2], step[3]))
        elif kind == "P":
            dispatch_partner(step[1])
        elif kind == "X":
            lo, hi = (far, rows) if step[2] else (0, reach[step[1]])
            where(lambda: experts(step[1], lo, hi, step == first))
        elif kind == "Y":
            reply(step[1])
        elif kind == "C":
            where(lambda: [combine(step[1], h) for h in range(pieces)] and None)
        elif kind == "CP":
            combine_partner(step[1])
        elif kind == "CR":
            for h in range(pieces):
                combine(step[1], h)
                reduce(step[1], h, side)
            for h in range(pieces):
                reduce(step[1], h, -side)
        elif kind == "R":
            for way in (side, -side):
                for h in range(pieces):
                    reduce(step[1], h, way)
        else:
            ends = home_partner if step[1] else home
            where(lambda: [ends(h) for h in range(pieces)] and None)

    steps = plan(chips, per)
    first = next(step for step in steps if step[0] == "X")
    for step in steps:
        with jax.named_scope("_".join(str(s) for s in step)):
            run(step)

    with jax.named_scope("settle"):
        taken(meta.at[OWN, 0, 0], m_send.at[0])
        taken(meta.at[OWN, :chips - 1], m_send.at[1])
        for i in range(chunks):
            taken(xs.at[i, :reach[i] - 1], y_send.at[i])
        taken(pr.at[OWN], p_send.at[chips])
        taken(zr.at[:chips - 1], z_send.at[0])
        pltpu.make_async_copy(out_ref, out_hbm, out_sem.at[0]).wait()
        if shared:
            taken(meta.at[PAR], m_send.at[2])
            heard(PAR, chunks - 1)
            taken(pr.at[PAR, chip], p_send.at[chip])
            taken(dr, d_send.at[0])
            for i in range(2):
                on_mid(lambda: lent(i).wait_send())
                on_edge(lambda: repaid(i).wait_send())
            for i in (1, 2):
                on_mid(lambda: taken(pr.at[PAR, order[i]], p_send.at[order[i]]))
                on_mid(lambda: taken(pz, d_send.at[i]))


def body(tokens, expert_ids, gate_probs, w_gate, w_up, w_down):
    count, choices = expert_ids.shape
    width = tokens.shape[1]
    hidden = w_gate.shape[2]
    rows = lax.axis_size("row")
    cols = lax.axis_size("col")
    slots = 5 * count * choices // (4 * rows * cols * w_gate.shape[0])
    group = 2
    while group * slots % 16:
        group *= 2
    chips = cols // 2
    chunks = chips // (group // 2)
    part = group * slots
    any_spec = pl.BlockSpec(memory_space=pl.ANY)
    dma = pltpu.SemaphoreType.DMA
    kinds = 2 if staged(chips, group // 2) else 1
    scratch = [
        pltpu.VMEM((count, width), BF16),
        pltpu.VMEM((choices, count), jnp.int32),
        pltpu.VMEM((choices, count), F32),
        pltpu.VMEM((kinds, chips, 2, 2 * choices, count), F32),
        pltpu.VMEM((kinds, chips, 2, count, width), BF16),
        pltpu.VMEM((width, hidden), BF16),
        pltpu.VMEM((width, hidden), BF16),
        pltpu.VMEM((hidden, width), BF16),
        pltpu.VMEM(((rows + 2) * part, group * count), BF16),
        pltpu.VMEM((chunks, (rows + 2) * part, group * count), BF16),
        pltpu.VMEM((rows * part, hidden), BF16),
        pltpu.VMEM((chunks, rows - 1, part, width), BF16),
        pltpu.VMEM((chunks, rows, part, width), BF16),
        pltpu.VMEM((chunks, rows + 2, part, width), BF16),
        pltpu.VMEM((kinds, chips, count, width), BF16),
        pltpu.VMEM((chips + 1, count, width), BF16),
        pltpu.VMEM((2, part, width), BF16),
        pltpu.VMEM((count, width), BF16),
        pltpu.VMEM((count, width), BF16),
        dma((6,)),
        dma((3,)), dma((kinds, chips)),
        dma((1,)), dma((1,)),
        dma((chips + 1,)), dma((chips, HALVES)),
        dma((1,)), dma((chips,)),
        dma((kinds, chips)), dma((chips, HALVES)), dma((chips,)),
        dma((chunks,)), dma((chunks,)),
        dma((chunks,)), dma((chunks, PIECES)),
        dma((chips + 1,)), dma((chips, PIECES)), dma((chips,)),
        dma((1,)), dma((chips + 1, PIECES)),
        dma((2,)), dma((2,)),
        dma((2,)), dma((2,)),
        dma((3,)), dma((PIECES,)), dma((1,)), dma((1,)),
    ]
    return pl.pallas_call(
        functools.partial(moe_kernel, rows, cols, slots, group, PIECES),
        out_shape=jax.ShapeDtypeStruct((count, width), BF16),
        in_specs=[any_spec] * 6,
        out_specs=pl.BlockSpec(memory_space=pl.ANY),
        scratch_shapes=scratch,
        compiler_params=pltpu.CompilerParams(
            collective_id=0, has_side_effects=True, vmem_limit_bytes=67043328
        ),
    )(expert_ids.T, gate_probs.T, tokens, w_gate, w_up, w_down)


def solution(mesh):
    in_specs = (
        P(("row", "col"), None),
        P(("row", "col"), None),
        P(("row", "col"), None),
        P(("row", "col"), None, None),
        P(("row", "col"), None, None),
        P(("row", "col"), None, None),
    )
    out_specs = P(("row", "col"), None)
    return jax.shard_map(body, mesh=mesh, in_specs=in_specs, out_specs=out_specs, check_vma=False)
```

```python
import functools
import math

import jax
import jax.numpy as jnp
from jax import lax
from jax.experimental import pallas as pl
from jax.experimental.pallas import tpu as pltpu
from jax.sharding import PartitionSpec as P

MESH = pl.DeviceIdType.MESH
BF16 = jnp.bfloat16
F32 = jnp.float32
PIECES = 4
HALVES = 2
OWN, PAR = 0, 1


def flip(r, j):
    out, bit = r, 1
    while bit <= j:
        if j & bit:
            out = out + bit * (1 - 2 * ((r // bit) % 2))
        bit *= 2
    return out


def staged(chips, per):
    return per == 1 and chips == 4


def plan(chips, per):
    hops = range(1, chips)
    every = range(chips // per)
    halves = range(HALVES)
    if not staged(chips, per):
        return (
            [("A", OWN, d, h, "all") for d in hops for h in halves]
            + [("D", i, h) for i in every for h in halves]
            + [step for i in every for step in (("X", i, 0, "all"), ("Y", i))]
            + [("C", i, "all") for i in every] + [("R", k) for k in hops] + [("H", OWN, "all")]
        )
    steps = [("S",), ("D", 0, 0), ("D", 0, 1)]
    for h in halves:
        steps += [("A", OWN, 1, h, "all"), ("A", OWN, 2, h, "mid"), ("D", 1, h)]
    steps += [("T", 0, 0), ("T", 0, 1), ("A", PAR, 0, 0, "all"), ("P", 0)]
    steps += [("A", OWN, 3, 0, "mid"), ("X", 1, 0, "all"), ("Y", 1), ("A", OWN, 3, 1, "mid")]
    for h in halves:
        steps += [("A", OWN, 2, h, "end"), ("D", 2, h)]
    steps += [("L", 0), ("X", 0, 0, "all")]
    steps += [("D", 3, 0, "mid"), ("D", 3, 1, "mid"), ("CR", 1)]
    for h in halves:
        steps += [("A", OWN, 3, h, "end"), ("D", 3, h, "end")]
    return steps + [
        ("A", PAR, 1, 0, "mid"), ("P", 1), ("L", 1),
        ("X", 2, 0, "all"), ("Y", 2), ("X", 1, 1, "all"),
        ("A", PAR, 2, 0, "mid"), ("CP", 1, "mid"), ("P", 2),
        ("X", 2, 1, "all"), ("X", 3, 0, "all"), ("Y", 3), ("Y", 0), ("X", 0, 1, "mid"),
        ("CP", 2, "mid"), ("CP", 0, "mid"), ("CR", 2), ("X", 0, 1, "end"), ("CP", 0, "end"),
        ("H", PAR, "mid"), ("CR", 3),
        ("H", PAR, "end"), ("C", 0, "all"), ("H", OWN, "all"),
    ]


def moe_kernel(
    rows, cols, slots, group, pieces,
    ids_in, probs_in, tok_in, wg_in, wu_in, wd_in, out_hbm,
    out_ref, ids_v, probs_v, meta, tok, wg, wu, wd, disp, comb, hid, xs, xr, yr, pr, zr, es, pz, dr,
    load_sem, m_send, m_recv, pt_send, pt_recv, ztok_send, ztok_recv, gtok_send, gtok_recv,
    ctok_send, ctok_recv, stok_recv, x_send, x_recv, y_send, y_recv, p_send, p_recv, g_recv,
    z_send, z_recv, e_send, e_recv, q_send, q_recv, d_send, d_recv, pz_recv, out_sem,
):
    r = lax.axis_index("row")
    c = lax.axis_index("col")
    chips = cols // 2
    chip, core = c // 2, c % 2
    mate = 2 * chip + (1 - core)
    far = rows - 1
    partner = flip(r, far)
    count, width = tok_in.shape
    choices = ids_in.shape[0]
    per = group // 2
    chunks = chips // per
    part = group * slots
    shared = staged(chips, per)
    modes = (OWN, PAR) if shared else (OWN,)
    reach = [far if shared and i < chunks - 1 else rows for i in range(chunks)]
    hidden = wg.shape[1]
    f_tile = math.gcd(hidden, 256)
    d_tile = math.gcd(width // pieces, 512)
    piece = width // pieces
    half = width // HALVES

    def remote(src, dst, send, recv, row, col):
        return pltpu.make_async_remote_copy(
            src_ref=src, dst_ref=dst, send_sem=send, recv_sem=recv,
            device_id=(row, col), device_id_type=MESH,
        )

    def taken(ref, sem):
        pltpu.make_async_copy(ref, ref, sem).wait()

    short = jnp.minimum(chip, chips - 1 - chip)
    side = jnp.where(2 * chip < chips, 1, -1)
    inner = 2 * (chip + side) + core
    outer = 2 * ((chip - side + chips) % chips) + core
    across = 2 * ((chip + 2 * side + chips) % chips) + core
    edge = short == 0
    order, signs = [chip], [None]
    for p in range(1, chips):
        both = p <= 2 * short
        sign = jnp.where(both, side if p % 2 else -side, side)
        dist = jnp.where(both, (p + 1) // 2, p - short)
        order.append(chip + sign * dist)
        signs.append(sign)

    def on_edge(act):
        pl.when(edge)(act)

    def on_mid(act):
        pl.when(jnp.logical_not(edge))(act)

    load_tok = pltpu.make_async_copy(tok_in, tok.at[OWN, chip, 0], load_sem.at[0])
    load_ids = pltpu.make_async_copy(ids_in, ids_v, load_sem.at[1])
    load_probs = pltpu.make_async_copy(probs_in, probs_v, load_sem.at[5])
    load_w = [
        pltpu.make_async_copy(wg_in.at[0], wg, load_sem.at[2]),
        pltpu.make_async_copy(wu_in.at[0], wu, load_sem.at[3]),
        pltpu.make_async_copy(wd_in.at[0], wd, load_sem.at[4]),
    ]
    load_tok.start()
    load_ids.start()
    load_probs.start()

    barrier = pltpu.get_barrier_semaphore()
    for d in range(1, cols):
        for row in (r, partner)[:len(modes)]:
            pl.semaphore_signal(
                barrier, inc=1, device_id=(row, (c + d) % cols), device_id_type=MESH
            )
    for j in range(1, rows):
        pl.semaphore_signal(barrier, inc=1, device_id=(flip(r, j), c), device_id_type=MESH)
    load_ids.wait()
    load_probs.wait()
    meta[OWN, chip, 0, :choices] = ids_v[...].astype(F32)
    meta[OWN, chip, 0, choices:] = probs_v[...]
    pl.semaphore_wait(barrier, len(modes) * (cols - 1) + rows - 1)

    def hop(o, q, send, to, h):
        at = pl.ds(h * half, half) if o == OWN else pl.ds(0, width)
        return remote(
            tok.at[o, q, 0, :, at], tok.at[o, q, 0, :, at],
            ztok_send.at[send] if o == OWN else gtok_send.at[0],
            ztok_recv.at[q, h] if o == OWN else gtok_recv.at[q],
            r, 2 * ((to + chips) % chips) + core,
        )

    def sent(o, p):
        q = order[p]
        if o == PAR:
            if p == 0:
                taken(tok.at[PAR, q, 0], gtok_send.at[0])
        elif p == 0:
            pl.when(chip > 0)(lambda: taken(tok.at[OWN, q, 0], ztok_send.at[0]))
            pl.when(chip < chips - 1)(lambda: taken(tok.at[OWN, q, 0], ztok_send.at[chips]))
        else:
            to = chip - signs[p]
            pl.when((to >= 0) & (to < chips))(
                lambda: taken(tok.at[OWN, q, 0], ztok_send.at[p])
            )

    def onward(o, p, h, act):
        if o == PAR:
            if p == 0:
                act(hop(PAR, chip, 0, chip + side, h))
        elif p == 0:
            @pl.when(chip > 0)
            def _():
                act(hop(OWN, chip, 0, chip - 1, h))

            @pl.when(chip < chips - 1)
            def _():
                act(hop(OWN, chip, chips, chip + 1, h))
        else:
            to = chip - signs[p]

            @pl.when((to >= 0) & (to < chips))
            def _():
                act(hop(OWN, order[p], p, to, h))

    def swap(o, p, h):
        at = pl.ds(h * half, half) if o == OWN else pl.ds(0, width)
        return remote(
            tok.at[o, order[p], 0, :, at], tok.at[o, order[p], 1, :, at],
            ctok_send.at[o, p], ctok_recv.at[p, h] if o == OWN else stok_recv.at[p], r, mate,
        )

    def share():
        return remote(
            tok.at[OWN, chip, 0], tok.at[PAR, chip, 0], pt_send.at[0], pt_recv.at[0], partner, c
        )

    def routing(o, d, t, slot):
        dist, other = d // 2, d % 2
        to = 2 * t + (core if other == 0 else 1 - core)
        return remote(
            meta.at[OWN, chip, 0], meta.at[o, slot, other],
            m_send.at[2 if o else min(dist, 1)], m_recv.at[o, slot], partner if o else r, to,
        )

    for o in modes:
        for d in range(1 - o, cols):
            routing(o, d, (chip + d // 2) % chips, chip).start()
    load_tok.wait()
    for h in range(HALVES):
        swap(OWN, 0, h).start()
        onward(OWN, 0, h, lambda copy: copy.start())
    for copy in load_w:
        copy.start()
    earlier = (
        lax.broadcasted_iota(jnp.int32, (count, count), 0)
        < lax.broadcasted_iota(jnp.int32, (count, count), 1)
    ).astype(BF16)
    slot_of = lax.broadcasted_iota(jnp.int32, (part, count), 0).astype(F32)
    lane_rows = 16
    row_id = lax.broadcasted_iota(jnp.int32, (lane_rows, count), 0)

    def route(o, i, base, experts_of):
        for s in range(group):
            q = order[i * per + s // 2]
            ids = meta[o, q, s % 2, :choices].astype(jnp.int32)
            probs = meta[o, q, s % 2, choices:]
            named = jnp.zeros((lane_rows, count), F32)
            weights = []
            for j, expert in enumerate(experts_of):
                hit = (ids == expert).astype(F32)
                named = jnp.where(row_id == j, jnp.sum(hit, axis=0, keepdims=True), named)
                weights.append(jnp.sum(hit * probs, axis=0, keepdims=True))
            rank = jnp.dot(named.astype(BF16), earlier, preferred_element_type=F32)
            key = jnp.where(named > 0.5, rank + float(s * slots), -1.0)
            for j in range(len(experts_of)):
                one = (slot_of == key[j:j + 1, :]).astype(F32)
                at = pl.ds((base + j) * part, part)
                disp[at, s * count:(s + 1) * count] = one.astype(BF16)
                comb[i, at, s * count:(s + 1) * count] = (one * weights[j]).astype(BF16)


    def arrive(o, d, h):
        if o == PAR and d == 0:
            share().wait_recv()
        else:
            hop(o, order[d], d, chip, h).wait_recv()
        onward(o, d, h, lambda copy: copy.start())
        swap(o, d, h).start()

    def heard(o, i):
        for d in range(i * per, (i + 1) * per):
            home_only = o == OWN and d == 0
            taken(
                meta.at[o, order[d], 1] if home_only else meta.at[o, order[d]],
                m_recv.at[o, order[d]],
            )

    def blocks(o, i, at):
        return jnp.concatenate(
            [tok[o, q, :, :, at].reshape(2 * count, d_tile) for q in order[i * per:(i + 1) * per]]
        )

    def dispatch(i, h):
        if h == 0:
            heard(OWN, i)
            route(OWN, i, 0, [flip(r, j) * cols + c for j in range(reach[i])])
        for d in range(i * per, (i + 1) * per):
            swap(OWN, d, h).wait_recv()
        near = reach[i] * part

        def tile(n, _):
            at = pl.ds(pl.multiple_of(n * d_tile, d_tile), d_tile)
            res = jnp.dot(disp[:near], blocks(OWN, i, at), preferred_element_type=F32).astype(BF16)
            xr[i, 0, :, at] = res[:part]
            xs[i, :reach[i] - 1, :, at] = res[part:].reshape(reach[i] - 1, part, d_tile)
            return 0

        lax.fori_loop(h * half // d_tile, (h + 1) * half // d_tile, tile, 0)

    def slot_copy(i, j, h):
        at = pl.ds(h * half, half)
        return remote(
            xs.at[i, j - 1, :, at], xr.at[i, j, :, at],
            x_send.at[i], x_recv.at[i], flip(r, j), c,
        )

    def transmit(i, h):
        for j in range(1, reach[i]):
            slot_copy(i, j, h).start()

    def lent(i):
        return remote(es.at[i], xr.at[i + 1, far], e_send.at[i], e_recv.at[i], r, outer)

    def repaid(i):
        return remote(
            yr.at[i + 1, far], yr.at[0, rows + i], q_send.at[i], q_recv.at[i],
            r, across if i else inner,
        )

    def dispatch_partner(i):
        def work(lend):
            heard(PAR, i)
            mine = [r * cols + c] + ([r * cols + outer] if lend else [])
            route(PAR, i, far, mine + ([r * cols + across] if lend and i == 0 else []))
            swap(PAR, i, 0).wait_recv()

            def tile(n, _):
                at = pl.ds(pl.multiple_of(n * d_tile, d_tile), d_tile)
                res = jnp.dot(
                    disp[far * part:(far + len(mine)) * part], blocks(PAR, i, at),
                    preferred_element_type=F32,
                ).astype(BF16)
                xr[i, far, :, at] = res[:part]
                if lend:
                    es[i, :, at] = res[part:]
                return 0

            lax.fori_loop(0, width // d_tile, tile, 0)

        on_mid(lambda: work(i < 2))
        on_edge(lambda: heard(PAR, i) if i else work(False))

    def experts(i, lo, hi, first):
        if lo == 0:
            taken(xs.at[i, :hi - 1], x_send.at[i])
            taken(xr.at[i, 1:hi], x_recv.at[i])
        elif i:
            on_edge(lambda: lent(i - 1).wait_recv())
        if first:
            for copy in load_w:
                copy.wait()
        size = (hi - lo) * part

        def up_tile(n, _):
            at = pl.ds(pl.multiple_of(n * f_tile, f_tile), f_tile)
            x = xr[i, lo:hi].reshape(size, width)
            gate = jnp.dot(x, wg[:, at], preferred_element_type=F32)
            up = jnp.dot(x, wu[:, at], preferred_element_type=F32)
            hid[:size, at] = (gate / (1.0 + jnp.exp(-gate)) * up).astype(BF16)
            return 0

        lax.fori_loop(0, hidden // f_tile, up_tile, 0)

        def down_tile(n, _):
            at = pl.ds(pl.multiple_of(n * d_tile, d_tile), d_tile)
            res = jnp.dot(hid[:size], wd[:, at], preferred_element_type=F32).astype(BF16)
            if lo == 0:
                yr[i, 0, :, at] = res[:part]
                xs[i, :hi - 1, :, at] = res[part:].reshape(hi - 1, part, d_tile)
            else:
                yr[i, far, :, at] = res
            return 0

        lax.fori_loop(0, width // d_tile, down_tile, 0)
        if lo and i:
            on_edge(lambda: repaid(i - 1).start())

    def reply(i):
        for h in range(pieces):
            at = pl.ds(h * piece, piece)
            for j in range(1, reach[i]):
                remote(
                    xs.at[i, j - 1, :, at], yr.at[i, j, :, at],
                    y_send.at[i], y_recv.at[i, h], flip(r, j), c,
                ).start()

    def mate_copy(o, q, h):
        at = pl.ds(h * piece, piece)
        return remote(
            tok.at[o, q, 1, :, at], pr.at[o, q, :, at],
            p_send.at[q if o else chips], p_recv.at[q, h] if o == OWN else g_recv.at[q], r, mate,
        )

    def weigh(o, i, lo, hi, h):
        def tile(n, _):
            at = pl.ds(pl.multiple_of(n * d_tile, d_tile), d_tile)
            y = yr[i, lo:hi, :, at].reshape((hi - lo) * part, d_tile)
            res = lax.dot_general(
                comb[i, lo * part:hi * part], y, (((0,), (0,)), ((), ())),
                preferred_element_type=F32,
            ).astype(BF16)
            for p in range(per):
                q = order[i * per + p]
                tok[o, q, 0, :, at] = res[2 * p * count:(2 * p + 1) * count]
                tok[o, q, 1, :, at] = res[(2 * p + 1) * count:(2 * p + 2) * count]
            return 0

        lax.fori_loop(h * piece // d_tile, (h + 1) * piece // d_tile, tile, 0)
        for d in range(i * per, (i + 1) * per):
            mate_copy(o, order[d], h).start()

    def free(o, d):
        sent(o, d)
        if shared and o == OWN and d == 0:
            share().wait_send()
        taken(tok.at[o, order[d], 0], ctok_send.at[o, d])

    def combine(i, h):
        if h == 0:
            for d in range(i * per, (i + 1) * per):
                free(OWN, d)
        taken(yr.at[i, 1:reach[i], :, pl.ds(h * piece, piece)], y_recv.at[i, h])
        weigh(OWN, i, 0, reach[i], h)

    def combine_partner(i, role):
        def work(lent_out):
            free(PAR, i)
            for j in range(lent_out):
                repaid(j).wait_recv()
            for h in range(pieces):
                weigh(PAR, i, far, rows + lent_out, h)

        if role == "end":
            work(0)
        elif i == 0:
            work(2)
        else:
            work(0)
            give(i)

    def both_cores(o, q, h):
        at = pl.ds(h * piece, piece)
        return tok[o, q, 0, :, at].astype(F32) + pr[o, q, :, at].astype(F32)

    def given(q, i, h, col):
        at = pl.ds(h * piece, piece)
        return remote(
            tok.at[PAR, q, 0, :, at], pz.at[:, at], d_send.at[i], pz_recv.at[0], r, col
        )

    def give(i):
        q = order[i]
        taken(pr.at[PAR, q], g_recv.at[q])
        for h in range(pieces):
            at = pl.ds(h * piece, piece)
            tok[PAR, q, 0, :, at] = both_cores(PAR, q, h).astype(BF16)
            given(q, i, h, inner if i == 1 else outer).start()

    def chain(t, h, step):
        at = pl.ds(h * piece, piece)
        to = (chip + step + chips) % chips
        slot = jnp.where((to == t) & (step > 0), chips, t)
        return remote(
            tok.at[OWN, t, 0, :, at], zr.at[slot, :, at],
            z_send.at[0], z_recv.at[slot, h], r, 2 * to + core,
        )

    def landed(slot, h):
        at = pl.ds(h * piece, piece)
        remote(
            tok.at[OWN, chip, 0, :, at], zr.at[slot, :, at],
            z_send.at[0], z_recv.at[slot, h], r, mate,
        ).wait_recv()
        return zr[slot, :, at].astype(F32)

    def reduce(k, h, step):
        at = pl.ds(h * piece, piece)
        t = jnp.where(step > 0, k, chips - 1 - k)

        @pl.when((t - chip) * step > 0)
        def _():
            mate_copy(OWN, t, h).wait_recv()
            fed = chip != jnp.where(step > 0, 0, chips - 1)

            @pl.when(jnp.logical_not(fed))
            def _():
                tok[OWN, t, 0, :, at] = both_cores(OWN, t, h).astype(BF16)

            @pl.when(fed)
            def _():
                tok[OWN, t, 0, :, at] = (landed(t, h) + both_cores(OWN, t, h)).astype(BF16)

            chain(t, h, step).start()

    def back(h):
        at = pl.ds(h * piece, piece)
        return remote(
            tok.at[PAR, chip, 0, :, at], dr.at[:, at], d_send.at[0], d_recv.at[h], partner, c
        )

    def home_partner(h):
        at = pl.ds(h * piece, piece)
        if h == 0:
            taken(pr.at[PAR, chip], g_recv.at[chip])
            taken(pz, pz_recv.at[0])
        total = both_cores(PAR, chip, h) + pz[:, at].astype(F32)
        tok[PAR, chip, 0, :, at] = total.astype(BF16)
        back(h).start()

    def leave(h):
        at = pl.ds(h * piece, piece)
        return pltpu.make_async_copy(out_ref.at[:, at], out_hbm.at[:, at], out_sem.at[0])

    def home(h):
        at = pl.ds(h * piece, piece)
        mate_copy(OWN, chip, h).wait_recv()

        def finish(*slots_in):
            total = both_cores(OWN, chip, h)
            if shared:
                back(h).wait_recv()
                total = total + dr[:, at].astype(F32)
            for slot in slots_in:
                total = total + landed(slot, h)
            out_ref[:, at] = total.astype(BF16)

        pl.when(chip == 0)(lambda: finish(chip))
        pl.when(chip == chips - 1)(lambda: finish(chips))
        pl.when((chip > 0) & (chip < chips - 1))(lambda: finish(chip, chips))
        leave(h).start()

    def run(step):
        kind = step[0]
        where = {"mid": on_mid, "end": on_edge}.get(step[-1], lambda act: act())
        if kind == "S":
            share().start()
        elif kind == "D":
            def both():
                dispatch(step[1], step[2])
                if step[1] or not shared:
                    transmit(step[1], step[2])

            where(both)
        elif kind == "T":
            transmit(step[1], step[2])
        elif kind == "L":
            on_mid(lambda: lent(step[1]).start())
        elif kind == "A":
            where(lambda: arrive(step[1], step[2], step[3]))
        elif kind == "P":
            dispatch_partner(step[1])
        elif kind == "X":
            lo, hi = (far, rows) if step[2] else (0, reach[step[1]])
            where(lambda: experts(step[1], lo, hi, step == first))
        elif kind == "Y":
            reply(step[1])
        elif kind == "C":
            where(lambda: [combine(step[1], h) for h in range(pieces)] and None)
        elif kind == "CP":
            where(lambda: combine_partner(step[1], step[-1]))
        elif kind == "CR":
            lag = 0 if step[1] == chunks - 1 else 1
            for h in range(pieces + lag):
                if h < pieces:
                    combine(step[1], h)
                if h >= lag:
                    reduce(step[1], h - lag, side)
                if h > lag:
                    reduce(step[1], h - lag - 1, -side)
            reduce(step[1], pieces - 1, -side)
        elif kind == "R":
            for way in (side, -side):
                for h in range(pieces):
                    reduce(step[1], h, way)
        else:
            ends = home_partner if step[1] else home
            where(lambda: [ends(h) for h in range(pieces)] and None)

    steps = plan(chips, per)
    first = next(step for step in steps if step[0] == "X")
    for step in steps:
        with jax.named_scope("_".join(str(s) for s in step)):
            run(step)

    with jax.named_scope("settle"):
        taken(meta.at[OWN, 0, 0], m_send.at[0])
        taken(meta.at[OWN, :chips - 1], m_send.at[1])
        for i in range(chunks):
            taken(xs.at[i, :reach[i] - 1], y_send.at[i])
        taken(pr.at[OWN], p_send.at[chips])
        taken(zr.at[:chips - 1], z_send.at[0])
        pltpu.make_async_copy(out_ref, out_hbm, out_sem.at[0]).wait()
        if shared:
            taken(meta.at[PAR], m_send.at[2])
            heard(PAR, chunks - 1)
            taken(pr.at[PAR, chip], p_send.at[chip])
            taken(dr, d_send.at[0])
            for i in range(2):
                on_mid(lambda: lent(i).wait_send())
                on_edge(lambda: repaid(i).wait_send())
            for i in (1, 2):
                on_mid(lambda: taken(pr.at[PAR, order[i]], p_send.at[order[i]]))
                on_mid(lambda: taken(pz, d_send.at[i]))


def body(tokens, expert_ids, gate_probs, w_gate, w_up, w_down):
    count, choices = expert_ids.shape
    width = tokens.shape[1]
    hidden = w_gate.shape[2]
    rows = lax.axis_size("row")
    cols = lax.axis_size("col")
    slots = 5 * count * choices // (4 * rows * cols * w_gate.shape[0])
    group = 2
    while group * slots % 16:
        group *= 2
    chips = cols // 2
    chunks = chips // (group // 2)
    part = group * slots
    any_spec = pl.BlockSpec(memory_space=pl.ANY)
    dma = pltpu.SemaphoreType.DMA
    kinds = 2 if staged(chips, group // 2) else 1
    scratch = [
        pltpu.VMEM((count, width), BF16),
        pltpu.VMEM((choices, count), jnp.int32),
        pltpu.VMEM((choices, count), F32),
        pltpu.VMEM((kinds, chips, 2, 2 * choices, count), F32),
        pltpu.VMEM((kinds, chips, 2, count, width), BF16),
        pltpu.VMEM((width, hidden), BF16),
        pltpu.VMEM((width, hidden), BF16),
        pltpu.VMEM((hidden, width), BF16),
        pltpu.VMEM(((rows + 2) * part, group * count), BF16),
        pltpu.VMEM((chunks, (rows + 2) * part, group * count), BF16),
        pltpu.VMEM((rows * part, hidden), BF16),
        pltpu.VMEM((chunks, rows - 1, part, width), BF16),
        pltpu.VMEM((chunks, rows, part, width), BF16),
        pltpu.VMEM((chunks, rows + 2, part, width), BF16),
        pltpu.VMEM((kinds, chips, count, width), BF16),
        pltpu.VMEM((chips + 1, count, width), BF16),
        pltpu.VMEM((2, part, width), BF16),
        pltpu.VMEM((count, width), BF16),
        pltpu.VMEM((count, width), BF16),
        dma((6,)),
        dma((3,)), dma((kinds, chips)),
        dma((1,)), dma((1,)),
        dma((chips + 1,)), dma((chips, HALVES)),
        dma((1,)), dma((chips,)),
        dma((kinds, chips)), dma((chips, HALVES)), dma((chips,)),
        dma((chunks,)), dma((chunks,)),
        dma((chunks,)), dma((chunks, PIECES)),
        dma((chips + 1,)), dma((chips, PIECES)), dma((chips,)),
        dma((1,)), dma((chips + 1, PIECES)),
        dma((2,)), dma((2,)),
        dma((2,)), dma((2,)),
        dma((3,)), dma((PIECES,)), dma((1,)), dma((1,)),
    ]
    return pl.pallas_call(
        functools.partial(moe_kernel, rows, cols, slots, group, PIECES),
        out_shape=jax.ShapeDtypeStruct((count, width), BF16),
        in_specs=[any_spec] * 6,
        out_specs=pl.BlockSpec(memory_space=pl.ANY),
        scratch_shapes=scratch,
        compiler_params=pltpu.CompilerParams(
            collective_id=0, has_side_effects=True, vmem_limit_bytes=67043328
        ),
    )(expert_ids.T, gate_probs.T, tokens, w_gate, w_up, w_down)


def solution(mesh):
    in_specs = (
        P(("row", "col"), None),
        P(("row", "col"), None),
        P(("row", "col"), None),
        P(("row", "col"), None, None),
        P(("row", "col"), None, None),
        P(("row", "col"), None, None),
    )
    out_specs = P(("row", "col"), None)
    return jax.shard_map(body, mesh=mesh, in_specs=in_specs, out_specs=out_specs, check_vma=False)
```

```python
import functools
import math

import jax
import jax.numpy as jnp
from jax import lax
from jax.experimental import pallas as pl
from jax.experimental.pallas import tpu as pltpu
from jax.sharding import PartitionSpec as P

MESH = pl.DeviceIdType.MESH
BF16 = jnp.bfloat16
F32 = jnp.float32
SHARES = (2, 2, 2, 1, 1)
PIECES = len(SHARES)
HALVES = 2
OWN, PAR = 0, 1


def flip(r, j):
    out, bit = r, 1
    while bit <= j:
        if j & bit:
            out = out + bit * (1 - 2 * ((r // bit) % 2))
        bit *= 2
    return out


def staged(chips, per):
    return per == 1 and chips == 4


def plan(chips, per):
    hops = range(1, chips)
    every = range(chips // per)
    halves = range(HALVES)
    if not staged(chips, per):
        return (
            [("A", OWN, d, h, "all") for d in hops for h in halves]
            + [("D", i, h) for i in every for h in halves]
            + [step for i in every for step in (("X", i, 0, "all"), ("Y", i))]
            + [("C", i, "all") for i in every] + [("R", k) for k in hops] + [("H", OWN, "all")]
        )
    steps = [("S",), ("D", 0, 0), ("D", 0, 1)]
    for h in halves:
        steps += [("A", OWN, 1, h, "all"), ("A", OWN, 2, h, "mid"), ("D", 1, h)]
    steps += [("T", 0, 0), ("T", 0, 1), ("A", PAR, 0, 0, "all"), ("P", 0)]
    steps += [("A", OWN, 3, 0, "mid"), ("X", 1, 0, "all"), ("Y", 1), ("A", OWN, 3, 1, "mid")]
    for h in halves:
        steps += [("A", OWN, 2, h, "end"), ("D", 2, h)]
    steps += [("L", 0), ("X", 0, 0, "all")]
    steps += [("D", 3, 0, "mid"), ("D", 3, 1, "mid"), ("CR", 1)]
    for h in halves:
        steps += [("A", OWN, 3, h, "end"), ("D", 3, h, "end")]
    return steps + [
        ("A", PAR, 1, 0, "mid"), ("P", 1), ("L", 1),
        ("X", 2, 0, "all"), ("Y", 2), ("X", 1, 1, "all"),
        ("A", PAR, 2, 0, "mid"), ("CP", 1, "mid"), ("P", 2), ("G", 1),
        ("X", 2, 1, "all"), ("CP", 2, "mid"), ("X", 3, 0, "all"), ("Y", 3), ("Y", 0), ("G", 2),
        ("X", 0, 1, "mid"), ("CP", 0, "mid"), ("CR", 2), ("X", 0, 1, "end"), ("CP", 0, "end"),
        ("H", PAR, "mid"), ("CR", 3),
        ("H", PAR, "end"), ("C", 0, "all"), ("H", OWN, "all"),
    ]


def moe_kernel(
    rows, cols, slots, group, pieces,
    ids_in, probs_in, tok_in, wg_in, wu_in, wd_in, out_hbm,
    out_ref, ids_v, probs_v, meta, tok, wg, wu, wd, disp, comb, hid, xs, xr, yr, pr, zr, es, pz, dr,
    load_sem, m_send, m_recv, pt_send, pt_recv, ztok_send, ztok_recv, gtok_send, gtok_recv,
    ctok_send, ctok_recv, stok_recv, x_send, x_recv, y_send, y_recv, p_send, p_recv, g_recv,
    z_send, z_recv, e_send, e_recv, q_send, q_recv, d_send, d_recv, pz_recv, out_sem,
):
    r = lax.axis_index("row")
    c = lax.axis_index("col")
    chips = cols // 2
    chip, core = c // 2, c % 2
    mate = 2 * chip + (1 - core)
    far = rows - 1
    partner = flip(r, far)
    count, width = tok_in.shape
    choices = ids_in.shape[0]
    per = group // 2
    chunks = chips // per
    part = group * slots
    shared = staged(chips, per)
    modes = (OWN, PAR) if shared else (OWN,)
    reach = [far if shared and i < chunks - 1 else rows for i in range(chunks)]
    hidden = wg.shape[1]
    f_tile = math.gcd(hidden, 256)
    d_tile = math.gcd(width // HALVES, 512)
    unit = width // sum(SHARES)
    starts = [unit * sum(SHARES[:h]) for h in range(pieces + 1)]
    half = width // HALVES

    def cut(h):
        return pl.ds(starts[h], starts[h + 1] - starts[h])

    def remote(src, dst, send, recv, row, col):
        return pltpu.make_async_remote_copy(
            src_ref=src, dst_ref=dst, send_sem=send, recv_sem=recv,
            device_id=(row, col), device_id_type=MESH,
        )

    def taken(ref, sem):
        pltpu.make_async_copy(ref, ref, sem).wait()

    short = jnp.minimum(chip, chips - 1 - chip)
    side = jnp.where(2 * chip < chips, 1, -1)
    inner = 2 * (chip + side) + core
    outer = 2 * ((chip - side + chips) % chips) + core
    across = 2 * ((chip + 2 * side + chips) % chips) + core
    edge = short == 0
    order, signs = [chip], [None]
    for p in range(1, chips):
        both = p <= 2 * short
        sign = jnp.where(both, side if p % 2 else -side, side)
        dist = jnp.where(both, (p + 1) // 2, p - short)
        order.append(chip + sign * dist)
        signs.append(sign)

    def on_edge(act):
        pl.when(edge)(act)

    def on_mid(act):
        pl.when(jnp.logical_not(edge))(act)

    load_tok = pltpu.make_async_copy(tok_in, tok.at[OWN, chip, 0], load_sem.at[0])
    load_ids = pltpu.make_async_copy(ids_in, ids_v, load_sem.at[1])
    load_probs = pltpu.make_async_copy(probs_in, probs_v, load_sem.at[5])
    load_w = [
        pltpu.make_async_copy(wg_in.at[0], wg, load_sem.at[2]),
        pltpu.make_async_copy(wu_in.at[0], wu, load_sem.at[3]),
        pltpu.make_async_copy(wd_in.at[0], wd, load_sem.at[4]),
    ]
    load_tok.start()
    load_ids.start()
    load_probs.start()

    barrier = pltpu.get_barrier_semaphore()
    for d in range(1, cols):
        for row in (r, partner)[:len(modes)]:
            pl.semaphore_signal(
                barrier, inc=1, device_id=(row, (c + d) % cols), device_id_type=MESH
            )
    for j in range(1, rows):
        pl.semaphore_signal(barrier, inc=1, device_id=(flip(r, j), c), device_id_type=MESH)
    load_ids.wait()
    load_probs.wait()
    meta[OWN, chip, 0, :choices] = ids_v[...].astype(F32)
    meta[OWN, chip, 0, choices:] = probs_v[...]
    pl.semaphore_wait(barrier, len(modes) * (cols - 1) + rows - 1)

    def hop(o, q, send, to, h):
        at = pl.ds(h * half, half) if o == OWN else pl.ds(0, width)
        return remote(
            tok.at[o, q, 0, :, at], tok.at[o, q, 0, :, at],
            ztok_send.at[send] if o == OWN else gtok_send.at[0],
            ztok_recv.at[q, h] if o == OWN else gtok_recv.at[q],
            r, 2 * ((to + chips) % chips) + core,
        )

    def sent(o, p):
        q = order[p]
        if o == PAR:
            if p == 0:
                taken(tok.at[PAR, q, 0], gtok_send.at[0])
        elif p == 0:
            pl.when(chip > 0)(lambda: taken(tok.at[OWN, q, 0], ztok_send.at[0]))
            pl.when(chip < chips - 1)(lambda: taken(tok.at[OWN, q, 0], ztok_send.at[chips]))
        else:
            to = chip - signs[p]
            pl.when((to >= 0) & (to < chips))(
                lambda: taken(tok.at[OWN, q, 0], ztok_send.at[p])
            )

    def onward(o, p, h, act):
        if o == PAR:
            if p == 0:
                act(hop(PAR, chip, 0, chip + side, h))
        elif p == 0:
            @pl.when(chip > 0)
            def _():
                act(hop(OWN, chip, 0, chip - 1, h))

            @pl.when(chip < chips - 1)
            def _():
                act(hop(OWN, chip, chips, chip + 1, h))
        else:
            to = chip - signs[p]

            @pl.when((to >= 0) & (to < chips))
            def _():
                act(hop(OWN, order[p], p, to, h))

    def swap(o, p, h):
        at = pl.ds(h * half, half) if o == OWN else pl.ds(0, width)
        return remote(
            tok.at[o, order[p], 0, :, at], tok.at[o, order[p], 1, :, at],
            ctok_send.at[o, p], ctok_recv.at[p, h] if o == OWN else stok_recv.at[p], r, mate,
        )

    def share():
        return remote(
            tok.at[OWN, chip, 0], tok.at[PAR, chip, 0], pt_send.at[0], pt_recv.at[0], partner, c
        )

    def routing(o, d, t, slot):
        dist, other = d // 2, d % 2
        to = 2 * t + (core if other == 0 else 1 - core)
        return remote(
            meta.at[OWN, chip, 0], meta.at[o, slot, other],
            m_send.at[2 if o else min(dist, 1)], m_recv.at[o, slot], partner if o else r, to,
        )

    for o in modes:
        for d in range(1 - o, cols):
            routing(o, d, (chip + d // 2) % chips, chip).start()
    load_tok.wait()
    for h in range(HALVES):
        swap(OWN, 0, h).start()
        onward(OWN, 0, h, lambda copy: copy.start())
    for copy in load_w:
        copy.start()
    earlier = (
        lax.broadcasted_iota(jnp.int32, (count, count), 0)
        < lax.broadcasted_iota(jnp.int32, (count, count), 1)
    ).astype(BF16)
    slot_of = lax.broadcasted_iota(jnp.int32, (part, count), 0).astype(F32)
    lane_rows = 16
    row_id = lax.broadcasted_iota(jnp.int32, (lane_rows, count), 0)

    def route(o, i, base, experts_of):
        for s in range(group):
            q = order[i * per + s // 2]
            ids = meta[o, q, s % 2, :choices].astype(jnp.int32)
            probs = meta[o, q, s % 2, choices:]
            named = jnp.zeros((lane_rows, count), F32)
            weights = []
            for j, expert in enumerate(experts_of):
                hit = (ids == expert).astype(F32)
                named = jnp.where(row_id == j, jnp.sum(hit, axis=0, keepdims=True), named)
                weights.append(jnp.sum(hit * probs, axis=0, keepdims=True))
            rank = jnp.dot(named.astype(BF16), earlier, preferred_element_type=F32)
            key = jnp.where(named > 0.5, rank + float(s * slots), -1.0)
            for j in range(len(experts_of)):
                one = (slot_of == key[j:j + 1, :]).astype(F32)
                at = pl.ds((base + j) * part, part)
                disp[at, s * count:(s + 1) * count] = one.astype(BF16)
                comb[i, at, s * count:(s + 1) * count] = (one * weights[j]).astype(BF16)


    def arrive(o, d, h):
        if o == PAR and d == 0:
            share().wait_recv()
        else:
            hop(o, order[d], d, chip, h).wait_recv()
        onward(o, d, h, lambda copy: copy.start())
        swap(o, d, h).start()

    def heard(o, i):
        for d in range(i * per, (i + 1) * per):
            home_only = o == OWN and d == 0
            taken(
                meta.at[o, order[d], 1] if home_only else meta.at[o, order[d]],
                m_recv.at[o, order[d]],
            )

    def blocks(o, i, at):
        return jnp.concatenate(
            [tok[o, q, :, :, at].reshape(2 * count, d_tile) for q in order[i * per:(i + 1) * per]]
        )

    def dispatch(i, h):
        if h == 0:
            heard(OWN, i)
            route(OWN, i, 0, [flip(r, j) * cols + c for j in range(reach[i])])
        for d in range(i * per, (i + 1) * per):
            swap(OWN, d, h).wait_recv()
        near = reach[i] * part

        def tile(n, _):
            at = pl.ds(pl.multiple_of(n * d_tile, d_tile), d_tile)
            res = jnp.dot(disp[:near], blocks(OWN, i, at), preferred_element_type=F32).astype(BF16)
            xr[i, 0, :, at] = res[:part]
            xs[i, :reach[i] - 1, :, at] = res[part:].reshape(reach[i] - 1, part, d_tile)
            return 0

        lax.fori_loop(h * half // d_tile, (h + 1) * half // d_tile, tile, 0, unroll=True)

    def slot_copy(i, j, h):
        at = pl.ds(h * half, half)
        return remote(
            xs.at[i, j - 1, :, at], xr.at[i, j, :, at],
            x_send.at[i], x_recv.at[i], flip(r, j), c,
        )

    def transmit(i, h):
        for j in range(1, reach[i]):
            slot_copy(i, j, h).start()

    def lent(i):
        return remote(es.at[i], xr.at[i + 1, far], e_send.at[i], e_recv.at[i], r, outer)

    def repaid(i):
        return remote(
            yr.at[i + 1, far], yr.at[0, rows + i], q_send.at[i], q_recv.at[i],
            r, across if i else inner,
        )

    def dispatch_partner(i):
        def work(lend):
            heard(PAR, i)
            mine = [r * cols + c] + ([r * cols + outer] if lend else [])
            route(PAR, i, far, mine + ([r * cols + across] if lend and i == 0 else []))
            swap(PAR, i, 0).wait_recv()

            def tile(n, _):
                at = pl.ds(pl.multiple_of(n * d_tile, d_tile), d_tile)
                res = jnp.dot(
                    disp[far * part:(far + len(mine)) * part], blocks(PAR, i, at),
                    preferred_element_type=F32,
                ).astype(BF16)
                xr[i, far, :, at] = res[:part]
                if lend:
                    es[i, :, at] = res[part:]
                return 0

            lax.fori_loop(0, width // d_tile, tile, 0, unroll=True)

        on_mid(lambda: work(i < 2))
        on_edge(lambda: heard(PAR, i) if i else work(False))

    def experts(i, lo, hi, first):
        if lo == 0:
            taken(xs.at[i, :hi - 1], x_send.at[i])
            taken(xr.at[i, 1:hi], x_recv.at[i])
        elif i:
            on_edge(lambda: lent(i - 1).wait_recv())
        if first:
            for copy in load_w:
                copy.wait()
        size = (hi - lo) * part

        def up_tile(n, _):
            at = pl.ds(pl.multiple_of(n * f_tile, f_tile), f_tile)
            x = xr[i, lo:hi].reshape(size, width)
            gate = jnp.dot(x, wg[:, at], preferred_element_type=F32)
            up = jnp.dot(x, wu[:, at], preferred_element_type=F32)
            hid[:size, at] = (gate / (1.0 + jnp.exp(-gate)) * up).astype(BF16)
            return 0

        lax.fori_loop(0, hidden // f_tile, up_tile, 0, unroll=True)

        def down_tile(n, _):
            at = pl.ds(pl.multiple_of(n * d_tile, d_tile), d_tile)
            res = jnp.dot(hid[:size], wd[:, at], preferred_element_type=F32).astype(BF16)
            if lo == 0:
                yr[i, 0, :, at] = res[:part]
                xs[i, :hi - 1, :, at] = res[part:].reshape(hi - 1, part, d_tile)
            else:
                yr[i, far, :, at] = res
            return 0

        lax.fori_loop(0, width // d_tile, down_tile, 0, unroll=True)
        if lo and i:
            on_edge(lambda: repaid(i - 1).start())

    def reply(i):
        for h in range(pieces):
            at = cut(h)
            for j in range(1, reach[i]):
                remote(
                    xs.at[i, j - 1, :, at], yr.at[i, j, :, at],
                    y_send.at[i], y_recv.at[i, h], flip(r, j), c,
                ).start()

    def mate_copy(o, q, h):
        at = cut(h)
        return remote(
            tok.at[o, q, 1, :, at], pr.at[o, q, :, at],
            p_send.at[q if o else chips], p_recv.at[q, h] if o == OWN else g_recv.at[q], r, mate,
        )

    def weigh(o, i, lo, hi, h):
        c_tile = math.gcd(math.gcd(starts[h], starts[h + 1]), 512)

        def tile(n, _):
            at = pl.ds(pl.multiple_of(n * c_tile, c_tile), c_tile)
            y = yr[i, lo:hi, :, at].reshape((hi - lo) * part, c_tile)
            res = lax.dot_general(
                comb[i, lo * part:hi * part], y, (((0,), (0,)), ((), ())),
                preferred_element_type=F32,
            ).astype(BF16)
            for p in range(per):
                q = order[i * per + p]
                tok[o, q, 0, :, at] = res[2 * p * count:(2 * p + 1) * count]
                tok[o, q, 1, :, at] = res[(2 * p + 1) * count:(2 * p + 2) * count]
            return 0

        lax.fori_loop(starts[h] // c_tile, starts[h + 1] // c_tile, tile, 0, unroll=True)
        for d in range(i * per, (i + 1) * per):
            mate_copy(o, order[d], h).start()

    def free(o, d):
        sent(o, d)
        if shared and o == OWN and d == 0:
            share().wait_send()
        taken(tok.at[o, order[d], 0], ctok_send.at[o, d])

    def combine(i, h):
        if h == 0:
            for d in range(i * per, (i + 1) * per):
                free(OWN, d)
        taken(yr.at[i, 1:reach[i], :, cut(h)], y_recv.at[i, h])
        weigh(OWN, i, 0, reach[i], h)

    def combine_partner(i, role):
        def work(lent_out):
            free(PAR, i)
            for j in range(lent_out):
                repaid(j).wait_recv()
            for h in range(pieces):
                weigh(PAR, i, far, rows + lent_out, h)

        if role == "end":
            work(0)
        elif i == 0:
            work(2)
        else:
            work(0)

    def both_cores(o, q, h):
        at = cut(h)
        return tok[o, q, 0, :, at].astype(F32) + pr[o, q, :, at].astype(F32)

    def given(q, i, h, col):
        at = cut(h)
        return remote(
            tok.at[PAR, q, 0, :, at], pz.at[:, at], d_send.at[i], pz_recv.at[0], r, col
        )

    def give(i):
        q = order[i]
        taken(pr.at[PAR, q], g_recv.at[q])
        for h in range(pieces):
            at = cut(h)
            tok[PAR, q, 0, :, at] = both_cores(PAR, q, h).astype(BF16)
            given(q, i, h, inner if i == 1 else outer).start()

    def chain(t, h, step):
        at = cut(h)
        to = (chip + step + chips) % chips
        slot = jnp.where((to == t) & (step > 0), chips, t)
        return remote(
            tok.at[OWN, t, 0, :, at], zr.at[slot, :, at],
            z_send.at[0], z_recv.at[slot, h], r, 2 * to + core,
        )

    def landed(slot, h):
        at = cut(h)
        remote(
            tok.at[OWN, chip, 0, :, at], zr.at[slot, :, at],
            z_send.at[0], z_recv.at[slot, h], r, mate,
        ).wait_recv()
        return zr[slot, :, at].astype(F32)

    def reduce(k, h, step):
        at = cut(h)
        t = jnp.where(step > 0, k, chips - 1 - k)

        @pl.when((t - chip) * step > 0)
        def _():
            mate_copy(OWN, t, h).wait_recv()
            fed = chip != jnp.where(step > 0, 0, chips - 1)

            @pl.when(jnp.logical_not(fed))
            def _():
                tok[OWN, t, 0, :, at] = both_cores(OWN, t, h).astype(BF16)

            @pl.when(fed)
            def _():
                tok[OWN, t, 0, :, at] = (landed(t, h) + both_cores(OWN, t, h)).astype(BF16)

            chain(t, h, step).start()

    def back(h):
        at = cut(h)
        return remote(
            tok.at[PAR, chip, 0, :, at], dr.at[:, at], d_send.at[0], d_recv.at[h], partner, c
        )

    def home_partner(h):
        at = cut(h)
        if h == 0:
            taken(pr.at[PAR, chip], g_recv.at[chip])
            taken(pz, pz_recv.at[0])
        total = both_cores(PAR, chip, h) + pz[:, at].astype(F32)
        tok[PAR, chip, 0, :, at] = total.astype(BF16)
        back(h).start()

    def leave(h):
        at = cut(h)
        return pltpu.make_async_copy(out_ref.at[:, at], out_hbm.at[:, at], out_sem.at[0])

    def home(h):
        at = cut(h)
        mate_copy(OWN, chip, h).wait_recv()

        def finish(*slots_in):
            total = both_cores(OWN, chip, h)
            if shared:
                back(h).wait_recv()
                total = total + dr[:, at].astype(F32)
            for slot in slots_in:
                total = total + landed(slot, h)
            out_ref[:, at] = total.astype(BF16)

        pl.when(chip == 0)(lambda: finish(chip))
        pl.when(chip == chips - 1)(lambda: finish(chips))
        pl.when((chip > 0) & (chip < chips - 1))(lambda: finish(chip, chips))
        leave(h).start()

    def run(step):
        kind = step[0]
        where = {"mid": on_mid, "end": on_edge}.get(step[-1], lambda act: act())
        if kind == "S":
            share().start()
        elif kind == "D":
            def both():
                dispatch(step[1], step[2])
                if step[1] or not shared:
                    transmit(step[1], step[2])

            where(both)
        elif kind == "T":
            transmit(step[1], step[2])
        elif kind == "L":
            on_mid(lambda: lent(step[1]).start())
        elif kind == "A":
            where(lambda: arrive(step[1], step[2], step[3]))
        elif kind == "P":
            dispatch_partner(step[1])
        elif kind == "X":
            lo, hi = (far, rows) if step[2] else (0, reach[step[1]])
            where(lambda: experts(step[1], lo, hi, step == first))
        elif kind == "Y":
            reply(step[1])
        elif kind == "C":
            where(lambda: [combine(step[1], h) for h in range(pieces)] and None)
        elif kind == "CP":
            where(lambda: combine_partner(step[1], step[-1]))
        elif kind == "G":
            on_mid(lambda: give(step[1]))
        elif kind == "CR":
            if step[1] < chunks - 1:
                for h in range(pieces + 1):
                    if h < pieces:
                        combine(step[1], h)
                    if h:
                        reduce(step[1], h - 1, side)
                for h in range(pieces):
                    reduce(step[1], h, -side)
            else:
                turns = [(starts[h + 1] / unit, h, side) for h in range(pieces)]
                turns += [(due + SHARES[h] + 1.8, h, -side) for due, h, _ in turns]
                for _, h, way in sorted(turns, key=lambda turn: turn[:2]):
                    if way is side:
                        combine(step[1], h)
                    reduce(step[1], h, way)
        elif kind == "R":
            for way in (side, -side):
                for h in range(pieces):
                    reduce(step[1], h, way)
        else:
            ends = home_partner if step[1] else home
            where(lambda: [ends(h) for h in range(pieces)] and None)

    steps = plan(chips, per)
    first = next(step for step in steps if step[0] == "X")
    for step in steps:
        with jax.named_scope("_".join(str(s) for s in step)):
            run(step)

    with jax.named_scope("settle"):
        taken(meta.at[OWN, 0, 0], m_send.at[0])
        taken(meta.at[OWN, :chips - 1], m_send.at[1])
        for i in range(chunks):
            taken(xs.at[i, :reach[i] - 1], y_send.at[i])
        taken(pr.at[OWN], p_send.at[chips])
        taken(zr.at[:chips - 1], z_send.at[0])
        pltpu.make_async_copy(out_ref, out_hbm, out_sem.at[0]).wait()
        if shared:
            taken(meta.at[PAR], m_send.at[2])
            heard(PAR, chunks - 1)
            taken(pr.at[PAR, chip], p_send.at[chip])
            taken(dr, d_send.at[0])
            for i in range(2):
                on_mid(lambda: lent(i).wait_send())
                on_edge(lambda: repaid(i).wait_send())
            for i in (1, 2):
                on_mid(lambda: taken(pr.at[PAR, order[i]], p_send.at[order[i]]))
                on_mid(lambda: taken(pz, d_send.at[i]))


def body(tokens, expert_ids, gate_probs, w_gate, w_up, w_down):
    count, choices = expert_ids.shape
    width = tokens.shape[1]
    hidden = w_gate.shape[2]
    rows = lax.axis_size("row")
    cols = lax.axis_size("col")
    slots = 5 * count * choices // (4 * rows * cols * w_gate.shape[0])
    group = 2
    while group * slots % 16:
        group *= 2
    chips = cols // 2
    chunks = chips // (group // 2)
    part = group * slots
    any_spec = pl.BlockSpec(memory_space=pl.ANY)
    dma = pltpu.SemaphoreType.DMA
    kinds = 2 if staged(chips, group // 2) else 1
    scratch = [
        pltpu.VMEM((count, width), BF16),
        pltpu.VMEM((choices, count), jnp.int32),
        pltpu.VMEM((choices, count), F32),
        pltpu.VMEM((kinds, chips, 2, 2 * choices, count), F32),
        pltpu.VMEM((kinds, chips, 2, count, width), BF16),
        pltpu.VMEM((width, hidden), BF16),
        pltpu.VMEM((width, hidden), BF16),
        pltpu.VMEM((hidden, width), BF16),
        pltpu.VMEM(((rows + 2) * part, group * count), BF16),
        pltpu.VMEM((chunks, (rows + 2) * part, group * count), BF16),
        pltpu.VMEM((rows * part, hidden), BF16),
        pltpu.VMEM((chunks, rows - 1, part, width), BF16),
        pltpu.VMEM((chunks, rows, part, width), BF16),
        pltpu.VMEM((chunks, rows + 2, part, width), BF16),
        pltpu.VMEM((kinds, chips, count, width), BF16),
        pltpu.VMEM((chips + 1, count, width), BF16),
        pltpu.VMEM((2, part, width), BF16),
        pltpu.VMEM((count, width), BF16),
        pltpu.VMEM((count, width), BF16),
        dma((6,)),
        dma((3,)), dma((kinds, chips)),
        dma((1,)), dma((1,)),
        dma((chips + 1,)), dma((chips, HALVES)),
        dma((1,)), dma((chips,)),
        dma((kinds, chips)), dma((chips, HALVES)), dma((chips,)),
        dma((chunks,)), dma((chunks,)),
        dma((chunks,)), dma((chunks, PIECES)),
        dma((chips + 1,)), dma((chips, PIECES)), dma((chips,)),
        dma((1,)), dma((chips + 1, PIECES)),
        dma((2,)), dma((2,)),
        dma((2,)), dma((2,)),
        dma((3,)), dma((PIECES,)), dma((1,)), dma((1,)),
    ]
    return pl.pallas_call(
        functools.partial(moe_kernel, rows, cols, slots, group, PIECES),
        out_shape=jax.ShapeDtypeStruct((count, width), BF16),
        in_specs=[any_spec] * 6,
        out_specs=pl.BlockSpec(memory_space=pl.ANY),
        scratch_shapes=scratch,
        compiler_params=pltpu.CompilerParams(
            collective_id=0, has_side_effects=True, vmem_limit_bytes=67043328
        ),
    )(expert_ids.T, gate_probs.T, tokens, w_gate, w_up, w_down)


def solution(mesh):
    in_specs = (
        P(("row", "col"), None),
        P(("row", "col"), None),
        P(("row", "col"), None),
        P(("row", "col"), None, None),
        P(("row", "col"), None, None),
        P(("row", "col"), None, None),
    )
    out_specs = P(("row", "col"), None)
    return jax.shard_map(body, mesh=mesh, in_specs=in_specs, out_specs=out_specs, check_vma=False)
```

```python
import functools
import math

import jax
import jax.numpy as jnp
from jax import lax
from jax.experimental import pallas as pl
from jax.experimental.pallas import tpu as pltpu
from jax.sharding import PartitionSpec as P

MESH = pl.DeviceIdType.MESH
BF16 = jnp.bfloat16
F32 = jnp.float32
SHARES = (2, 2, 2, 1, 1)
PIECES = len(SHARES)
HALVES = 2
OWN, PAR = 0, 1


def flip(r, j):
    out, bit = r, 1
    while bit <= j:
        if j & bit:
            out = out + bit * (1 - 2 * ((r // bit) % 2))
        bit *= 2
    return out


def staged(chips, per):
    return per == 1 and chips == 4


def plan(chips, per):
    hops = range(1, chips)
    every = range(chips // per)
    halves = range(HALVES)
    if not staged(chips, per):
        return (
            [("A", OWN, d, h, "all") for d in hops for h in halves]
            + [("D", i, h) for i in every for h in halves]
            + [step for i in every for step in (("X", i, 0, "all"), ("Y", i))]
            + [("C", i, "all") for i in every] + [("R", k) for k in hops] + [("H", OWN, "all")]
        )
    steps = [("S",), ("D", 0, 0), ("D", 0, 1)]
    for h in halves:
        steps += [("A", OWN, 1, h, "all"), ("A", OWN, 2, h, "mid"), ("D", 1, h)]
    steps += [("T", 0, 0), ("T", 0, 1), ("A", PAR, 0, 0, "all"), ("P", 0)]
    steps += [("A", OWN, 3, 0, "mid"), ("X", 1, 0, "all"), ("Y", 1), ("A", OWN, 3, 1, "mid")]
    for h in halves:
        steps += [("A", OWN, 2, h, "end"), ("D", 2, h)]
    steps += [("L", 0), ("X", 0, 0, "all")]
    steps += [("D", 3, 0, "mid"), ("D", 3, 1, "mid")]
    steps += [("A", OWN, 3, 0, "end"), ("D", 3, 0, "end"), ("CR", 1)]
    steps += [("A", OWN, 3, 1, "end"), ("D", 3, 1, "end")]
    return steps + [
        ("A", PAR, 1, 0, "mid"), ("P", 1), ("L", 1),
        ("X", 2, 0, "all"), ("Y", 2), ("X", 1, 1, "all"),
        ("A", PAR, 2, 0, "mid"), ("CP", 1, "mid"), ("P", 2), ("G", 1),
        ("X", 2, 1, "all"), ("CP", 2, "mid"), ("X", 3, 0, "all"), ("Y", 3), ("Y", 0), ("G", 2),
        ("X", 0, 1, "mid"), ("CP", 0, "mid"), ("CR", 2), ("X", 0, 1, "end"), ("CP", 0, "end"),
        ("H", PAR, "mid"), ("CR", 3),
        ("H", PAR, "end"), ("C", 0, "all"), ("H", OWN, "all"),
    ]


def moe_kernel(
    rows, cols, slots, group, pieces,
    ids_in, probs_in, tok_in, wg_in, wu_in, wd_in, out_hbm,
    out_ref, ids_v, probs_v, meta, tok, wg, wu, wd, disp, comb, hid, xs, xr, yr, pr, zr, es, pz, dr,
    load_sem, m_send, m_recv, pt_send, pt_recv, ztok_send, ztok_recv, gtok_send, gtok_recv,
    ctok_send, ctok_recv, stok_recv, x_send, x_recv, y_send, y_recv, p_send, p_recv, g_recv,
    z_send, z_recv, e_send, e_recv, q_send, q_recv, d_send, d_recv, pz_recv, out_sem,
):
    r = lax.axis_index("row")
    c = lax.axis_index("col")
    chips = cols // 2
    chip, core = c // 2, c % 2
    mate = 2 * chip + (1 - core)
    far = rows - 1
    partner = flip(r, far)
    count, width = tok_in.shape
    choices = ids_in.shape[0]
    per = group // 2
    chunks = chips // per
    part = group * slots
    shared = staged(chips, per)
    modes = (OWN, PAR) if shared else (OWN,)
    reach = [far if shared and i < chunks - 1 else rows for i in range(chunks)]
    hidden = wg.shape[1]
    f_tile = math.gcd(hidden, 256)
    d_tile = math.gcd(width // HALVES, 512)
    unit = width // sum(SHARES)
    starts = [unit * sum(SHARES[:h]) for h in range(pieces + 1)]
    half = width // HALVES

    def cut(h):
        return pl.ds(starts[h], starts[h + 1] - starts[h])

    def remote(src, dst, send, recv, row, col):
        return pltpu.make_async_remote_copy(
            src_ref=src, dst_ref=dst, send_sem=send, recv_sem=recv,
            device_id=(row, col), device_id_type=MESH,
        )

    def taken(ref, sem):
        pltpu.make_async_copy(ref, ref, sem).wait()

    short = jnp.minimum(chip, chips - 1 - chip)
    side = jnp.where(2 * chip < chips, 1, -1)
    inner = 2 * (chip + side) + core
    outer = 2 * ((chip - side + chips) % chips) + core
    across = 2 * ((chip + 2 * side + chips) % chips) + core
    edge = short == 0
    order, signs = [chip], [None]
    for p in range(1, chips):
        both = p <= 2 * short
        sign = jnp.where(both, side if p % 2 else -side, side)
        dist = jnp.where(both, (p + 1) // 2, p - short)
        order.append(chip + sign * dist)
        signs.append(sign)

    def on_edge(act):
        pl.when(edge)(act)

    def on_mid(act):
        pl.when(jnp.logical_not(edge))(act)

    load_tok = pltpu.make_async_copy(tok_in, tok.at[OWN, chip, 0], load_sem.at[0])
    load_ids = pltpu.make_async_copy(ids_in, ids_v, load_sem.at[1])
    load_probs = pltpu.make_async_copy(probs_in, probs_v, load_sem.at[5])
    load_w = [
        pltpu.make_async_copy(wg_in.at[0], wg, load_sem.at[2]),
        pltpu.make_async_copy(wu_in.at[0], wu, load_sem.at[3]),
        pltpu.make_async_copy(wd_in.at[0], wd, load_sem.at[4]),
    ]
    load_tok.start()
    load_ids.start()
    load_probs.start()

    barrier = pltpu.get_barrier_semaphore()
    for d in range(1, cols):
        for row in (r, partner)[:len(modes)]:
            pl.semaphore_signal(
                barrier, inc=1, device_id=(row, (c + d) % cols), device_id_type=MESH
            )
    for j in range(1, rows):
        pl.semaphore_signal(barrier, inc=1, device_id=(flip(r, j), c), device_id_type=MESH)
    load_ids.wait()
    load_probs.wait()
    meta[OWN, chip, 0, :choices] = ids_v[...].astype(F32)
    meta[OWN, chip, 0, choices:] = probs_v[...]
    pl.semaphore_wait(barrier, len(modes) * (cols - 1) + rows - 1)

    def hop(o, q, send, to, h):
        at = pl.ds(h * half, half) if o == OWN else pl.ds(0, width)
        return remote(
            tok.at[o, q, 0, :, at], tok.at[o, q, 0, :, at],
            ztok_send.at[send] if o == OWN else gtok_send.at[0],
            ztok_recv.at[q, h] if o == OWN else gtok_recv.at[q],
            r, 2 * ((to + chips) % chips) + core,
        )

    def sent(o, p):
        q = order[p]
        if o == PAR:
            if p == 0:
                taken(tok.at[PAR, q, 0], gtok_send.at[0])
        elif p == 0:
            pl.when(chip > 0)(lambda: taken(tok.at[OWN, q, 0], ztok_send.at[0]))
            pl.when(chip < chips - 1)(lambda: taken(tok.at[OWN, q, 0], ztok_send.at[chips]))
        else:
            to = chip - signs[p]
            pl.when((to >= 0) & (to < chips))(
                lambda: taken(tok.at[OWN, q, 0], ztok_send.at[p])
            )

    def onward(o, p, h, act):
        if o == PAR:
            if p == 0:
                act(hop(PAR, chip, 0, chip + side, h))
        elif p == 0:
            @pl.when(chip > 0)
            def _():
                act(hop(OWN, chip, 0, chip - 1, h))

            @pl.when(chip < chips - 1)
            def _():
                act(hop(OWN, chip, chips, chip + 1, h))
        else:
            to = chip - signs[p]

            @pl.when((to >= 0) & (to < chips))
            def _():
                act(hop(OWN, order[p], p, to, h))

    def swap(o, p, h):
        at = pl.ds(h * half, half) if o == OWN else pl.ds(0, width)
        return remote(
            tok.at[o, order[p], 0, :, at], tok.at[o, order[p], 1, :, at],
            ctok_send.at[o, p], ctok_recv.at[p, h] if o == OWN else stok_recv.at[p], r, mate,
        )

    def share():
        return remote(
            tok.at[OWN, chip, 0], tok.at[PAR, chip, 0], pt_send.at[0], pt_recv.at[0], partner, c
        )

    def routing(o, d, t, slot):
        dist, other = d // 2, d % 2
        to = 2 * t + (core if other == 0 else 1 - core)
        return remote(
            meta.at[OWN, chip, 0], meta.at[o, slot, other],
            m_send.at[2 if o else min(dist, 1)], m_recv.at[o, slot], partner if o else r, to,
        )

    for o in modes:
        for d in range(1 - o, cols):
            routing(o, d, (chip + d // 2) % chips, chip).start()
    load_tok.wait()
    for h in range(HALVES):
        swap(OWN, 0, h).start()
        onward(OWN, 0, h, lambda copy: copy.start())
    for copy in load_w:
        copy.start()
    earlier = (
        lax.broadcasted_iota(jnp.int32, (count, count), 0)
        < lax.broadcasted_iota(jnp.int32, (count, count), 1)
    ).astype(BF16)
    slot_of = lax.broadcasted_iota(jnp.int32, (part, count), 0).astype(F32)
    lane_rows = 16
    row_id = lax.broadcasted_iota(jnp.int32, (lane_rows, count), 0)

    def route(o, i, base, experts_of):
        for s in range(group):
            q = order[i * per + s // 2]
            ids = meta[o, q, s % 2, :choices].astype(jnp.int32)
            probs = meta[o, q, s % 2, choices:]
            named = jnp.zeros((lane_rows, count), F32)
            weights = []
            for j, expert in enumerate(experts_of):
                hit = (ids == expert).astype(F32)
                named = jnp.where(row_id == j, jnp.sum(hit, axis=0, keepdims=True), named)
                weights.append(jnp.sum(hit * probs, axis=0, keepdims=True))
            rank = jnp.dot(named.astype(BF16), earlier, preferred_element_type=F32)
            key = jnp.where(named > 0.5, rank + float(s * slots), -1.0)
            for j in range(len(experts_of)):
                one = (slot_of == key[j:j + 1, :]).astype(F32)
                at = pl.ds((base + j) * part, part)
                disp[at, s * count:(s + 1) * count] = one.astype(BF16)
                comb[i, at, s * count:(s + 1) * count] = (one * weights[j]).astype(BF16)


    def arrive(o, d, h):
        if o == PAR and d == 0:
            share().wait_recv()
        else:
            hop(o, order[d], d, chip, h).wait_recv()
        onward(o, d, h, lambda copy: copy.start())
        swap(o, d, h).start()

    def heard(o, i):
        for d in range(i * per, (i + 1) * per):
            home_only = o == OWN and d == 0
            taken(
                meta.at[o, order[d], 1] if home_only else meta.at[o, order[d]],
                m_recv.at[o, order[d]],
            )

    def blocks(o, i, at):
        return jnp.concatenate(
            [tok[o, q, :, :, at].reshape(2 * count, d_tile) for q in order[i * per:(i + 1) * per]]
        )

    def dispatch(i, h):
        if h == 0:
            heard(OWN, i)
            route(OWN, i, 0, [flip(r, j) * cols + c for j in range(reach[i])])
        for d in range(i * per, (i + 1) * per):
            swap(OWN, d, h).wait_recv()
        near = reach[i] * part

        def tile(n, _):
            at = pl.ds(pl.multiple_of(n * d_tile, d_tile), d_tile)
            res = jnp.dot(disp[:near], blocks(OWN, i, at), preferred_element_type=F32).astype(BF16)
            xr[i, 0, :, at] = res[:part]
            xs[i, :reach[i] - 1, :, at] = res[part:].reshape(reach[i] - 1, part, d_tile)
            return 0

        lax.fori_loop(h * half // d_tile, (h + 1) * half // d_tile, tile, 0, unroll=True)

    def slot_copy(i, j, h):
        at = pl.ds(h * half, half)
        return remote(
            xs.at[i, j - 1, :, at], xr.at[i, j, :, at],
            x_send.at[i], x_recv.at[i], flip(r, j), c,
        )

    def transmit(i, h):
        for j in range(1, reach[i]):
            slot_copy(i, j, h).start()

    def lent(i):
        return remote(es.at[i], xr.at[i + 1, far], e_send.at[i], e_recv.at[i], r, outer)

    def repaid(i):
        return remote(
            yr.at[i + 1, far], yr.at[0, rows + i], q_send.at[i], q_recv.at[i],
            r, across if i else inner,
        )

    def dispatch_partner(i):
        def work(lend):
            heard(PAR, i)
            mine = [r * cols + c] + ([r * cols + outer] if lend else [])
            route(PAR, i, far, mine + ([r * cols + across] if lend and i == 0 else []))
            swap(PAR, i, 0).wait_recv()

            def tile(n, _):
                at = pl.ds(pl.multiple_of(n * d_tile, d_tile), d_tile)
                res = jnp.dot(
                    disp[far * part:(far + len(mine)) * part], blocks(PAR, i, at),
                    preferred_element_type=F32,
                ).astype(BF16)
                xr[i, far, :, at] = res[:part]
                if lend:
                    es[i, :, at] = res[part:]
                return 0

            lax.fori_loop(0, width // d_tile, tile, 0, unroll=True)

        on_mid(lambda: work(i < 2))
        on_edge(lambda: heard(PAR, i) if i else work(False))

    def experts(i, lo, hi, first):
        if lo == 0:
            taken(xs.at[i, :hi - 1], x_send.at[i])
            taken(xr.at[i, 1:hi], x_recv.at[i])
        elif i:
            on_edge(lambda: lent(i - 1).wait_recv())
        if first:
            for copy in load_w:
                copy.wait()
        size = (hi - lo) * part

        def up_tile(n, _):
            at = pl.ds(pl.multiple_of(n * f_tile, f_tile), f_tile)
            x = xr[i, lo:hi].reshape(size, width)
            gate = jnp.dot(x, wg[:, at], preferred_element_type=F32)
            up = jnp.dot(x, wu[:, at], preferred_element_type=F32)
            hid[:size, at] = (gate / (1.0 + jnp.exp(-gate)) * up).astype(BF16)
            return 0

        lax.fori_loop(0, hidden // f_tile, up_tile, 0, unroll=True)

        def down_tile(n, _):
            at = pl.ds(pl.multiple_of(n * d_tile, d_tile), d_tile)
            res = jnp.dot(hid[:size], wd[:, at], preferred_element_type=F32).astype(BF16)
            if lo == 0:
                yr[i, 0, :, at] = res[:part]
                xs[i, :hi - 1, :, at] = res[part:].reshape(hi - 1, part, d_tile)
            else:
                yr[i, far, :, at] = res
            return 0

        lax.fori_loop(0, width // d_tile, down_tile, 0, unroll=True)
        if lo and i:
            on_edge(lambda: repaid(i - 1).start())

    def reply(i):
        for h in range(pieces):
            at = cut(h)
            for j in range(1, reach[i]):
                remote(
                    xs.at[i, j - 1, :, at], yr.at[i, j, :, at],
                    y_send.at[i], y_recv.at[i, h], flip(r, j), c,
                ).start()

    def mate_copy(o, q, h):
        at = cut(h)
        return remote(
            tok.at[o, q, 1, :, at], pr.at[o, q, :, at],
            p_send.at[q if o else chips], p_recv.at[q, h] if o == OWN else g_recv.at[q], r, mate,
        )

    def weigh(o, i, lo, hi, h):
        c_tile = math.gcd(math.gcd(starts[h], starts[h + 1]), 512)

        def tile(n, _):
            at = pl.ds(pl.multiple_of(n * c_tile, c_tile), c_tile)
            y = yr[i, lo:hi, :, at].reshape((hi - lo) * part, c_tile)
            res = lax.dot_general(
                comb[i, lo * part:hi * part], y, (((0,), (0,)), ((), ())),
                preferred_element_type=F32,
            ).astype(BF16)
            for p in range(per):
                q = order[i * per + p]
                tok[o, q, 0, :, at] = res[2 * p * count:(2 * p + 1) * count]
                tok[o, q, 1, :, at] = res[(2 * p + 1) * count:(2 * p + 2) * count]
            return 0

        lax.fori_loop(starts[h] // c_tile, starts[h + 1] // c_tile, tile, 0, unroll=True)
        for d in range(i * per, (i + 1) * per):
            mate_copy(o, order[d], h).start()

    def free(o, d):
        sent(o, d)
        if shared and o == OWN and d == 0:
            share().wait_send()
        taken(tok.at[o, order[d], 0], ctok_send.at[o, d])

    def combine(i, h):
        if h == 0:
            for d in range(i * per, (i + 1) * per):
                free(OWN, d)
        taken(yr.at[i, 1:reach[i], :, cut(h)], y_recv.at[i, h])
        weigh(OWN, i, 0, reach[i], h)

    def combine_partner(i, role):
        def work(lent_out):
            free(PAR, i)
            for j in range(lent_out):
                repaid(j).wait_recv()
            for h in range(pieces):
                weigh(PAR, i, far, rows + lent_out, h)

        if role == "end":
            work(0)
        elif i == 0:
            work(2)
        else:
            work(0)

    def both_cores(o, q, h):
        at = cut(h)
        return tok[o, q, 0, :, at].astype(F32) + pr[o, q, :, at].astype(F32)

    def given(q, i, h, col):
        at = cut(h)
        return remote(
            tok.at[PAR, q, 0, :, at], pz.at[:, at], d_send.at[i], pz_recv.at[0], r, col
        )

    def give(i):
        q = order[i]
        taken(pr.at[PAR, q], g_recv.at[q])
        for h in range(pieces):
            at = cut(h)
            tok[PAR, q, 0, :, at] = both_cores(PAR, q, h).astype(BF16)
            given(q, i, h, inner if i == 1 else outer).start()

    def chain(t, h, step):
        at = cut(h)
        to = (chip + step + chips) % chips
        slot = jnp.where((to == t) & (step > 0), chips, t)
        return remote(
            tok.at[OWN, t, 0, :, at], zr.at[slot, :, at],
            z_send.at[0], z_recv.at[slot, h], r, 2 * to + core,
        )

    def landed(slot, h):
        at = cut(h)
        remote(
            tok.at[OWN, chip, 0, :, at], zr.at[slot, :, at],
            z_send.at[0], z_recv.at[slot, h], r, mate,
        ).wait_recv()
        return zr[slot, :, at].astype(F32)

    def reduce(k, h, step):
        at = cut(h)
        t = jnp.where(step > 0, k, chips - 1 - k)

        @pl.when((t - chip) * step > 0)
        def _():
            mate_copy(OWN, t, h).wait_recv()
            fed = chip != jnp.where(step > 0, 0, chips - 1)

            @pl.when(jnp.logical_not(fed))
            def _():
                tok[OWN, t, 0, :, at] = both_cores(OWN, t, h).astype(BF16)

            @pl.when(fed)
            def _():
                tok[OWN, t, 0, :, at] = (landed(t, h) + both_cores(OWN, t, h)).astype(BF16)

            chain(t, h, step).start()

    def back(h):
        at = cut(h)
        return remote(
            tok.at[PAR, chip, 0, :, at], dr.at[:, at], d_send.at[0], d_recv.at[h], partner, c
        )

    def home_partner(h):
        at = cut(h)
        if h == 0:
            taken(pr.at[PAR, chip], g_recv.at[chip])
            taken(pz, pz_recv.at[0])
        total = both_cores(PAR, chip, h) + pz[:, at].astype(F32)
        tok[PAR, chip, 0, :, at] = total.astype(BF16)
        back(h).start()

    def leave(h):
        at = cut(h)
        return pltpu.make_async_copy(out_ref.at[:, at], out_hbm.at[:, at], out_sem.at[0])

    def home(h):
        at = cut(h)
        mate_copy(OWN, chip, h).wait_recv()

        def finish(*slots_in):
            total = both_cores(OWN, chip, h)
            if shared:
                back(h).wait_recv()
                total = total + dr[:, at].astype(F32)
            for slot in slots_in:
                total = total + landed(slot, h)
            out_ref[:, at] = total.astype(BF16)

        pl.when(chip == 0)(lambda: finish(chip))
        pl.when(chip == chips - 1)(lambda: finish(chips))
        pl.when((chip > 0) & (chip < chips - 1))(lambda: finish(chip, chips))
        leave(h).start()

    def run(step):
        kind = step[0]
        where = {"mid": on_mid, "end": on_edge}.get(step[-1], lambda act: act())
        if kind == "S":
            share().start()
        elif kind == "D":
            def both():
                dispatch(step[1], step[2])
                if step[1] or not shared:
                    transmit(step[1], step[2])

            where(both)
        elif kind == "T":
            transmit(step[1], step[2])
        elif kind == "L":
            on_mid(lambda: lent(step[1]).start())
        elif kind == "A":
            where(lambda: arrive(step[1], step[2], step[3]))
        elif kind == "P":
            dispatch_partner(step[1])
        elif kind == "X":
            lo, hi = (far, rows) if step[2] else (0, reach[step[1]])
            where(lambda: experts(step[1], lo, hi, step == first))
        elif kind == "Y":
            reply(step[1])
        elif kind == "C":
            where(lambda: [combine(step[1], h) for h in range(pieces)] and None)
        elif kind == "CP":
            where(lambda: combine_partner(step[1], step[-1]))
        elif kind == "G":
            on_mid(lambda: give(step[1]))
        elif kind == "CR":
            if step[1] < chunks - 1:
                for h in range(pieces + 1):
                    if h < pieces:
                        combine(step[1], h)
                    if h:
                        reduce(step[1], h - 1, side)
                for h in range(pieces):
                    reduce(step[1], h, -side)
            else:
                turns = [(starts[h + 1] / unit, h, side) for h in range(pieces)]
                turns += [(due + SHARES[h] + 1.8, h, -side) for due, h, _ in turns]
                for _, h, way in sorted(turns, key=lambda turn: turn[:2]):
                    if way is side:
                        combine(step[1], h)
                    reduce(step[1], h, way)
        elif kind == "R":
            for way in (side, -side):
                for h in range(pieces):
                    reduce(step[1], h, way)
        else:
            ends = home_partner if step[1] else home
            where(lambda: [ends(h) for h in range(pieces)] and None)

    steps = plan(chips, per)
    first = next(step for step in steps if step[0] == "X")
    for step in steps:
        with jax.named_scope("_".join(str(s) for s in step)):
            run(step)

    with jax.named_scope("settle"):
        taken(meta.at[OWN, 0, 0], m_send.at[0])
        taken(meta.at[OWN, :chips - 1], m_send.at[1])
        for i in range(chunks):
            taken(xs.at[i, :reach[i] - 1], y_send.at[i])
        taken(pr.at[OWN], p_send.at[chips])
        taken(zr.at[:chips - 1], z_send.at[0])
        pltpu.make_async_copy(out_ref, out_hbm, out_sem.at[0]).wait()
        if shared:
            taken(meta.at[PAR], m_send.at[2])
            heard(PAR, chunks - 1)
            taken(pr.at[PAR, chip], p_send.at[chip])
            taken(dr, d_send.at[0])
            for i in range(2):
                on_mid(lambda: lent(i).wait_send())
                on_edge(lambda: repaid(i).wait_send())
            for i in (1, 2):
                on_mid(lambda: taken(pr.at[PAR, order[i]], p_send.at[order[i]]))
                on_mid(lambda: taken(pz, d_send.at[i]))


def body(tokens, expert_ids, gate_probs, w_gate, w_up, w_down):
    count, choices = expert_ids.shape
    width = tokens.shape[1]
    hidden = w_gate.shape[2]
    rows = lax.axis_size("row")
    cols = lax.axis_size("col")
    slots = 5 * count * choices // (4 * rows * cols * w_gate.shape[0])
    group = 2
    while group * slots % 16:
        group *= 2
    chips = cols // 2
    chunks = chips // (group // 2)
    part = group * slots
    any_spec = pl.BlockSpec(memory_space=pl.ANY)
    dma = pltpu.SemaphoreType.DMA
    kinds = 2 if staged(chips, group // 2) else 1
    scratch = [
        pltpu.VMEM((count, width), BF16),
        pltpu.VMEM((choices, count), jnp.int32),
        pltpu.VMEM((choices, count), F32),
        pltpu.VMEM((kinds, chips, 2, 2 * choices, count), F32),
        pltpu.VMEM((kinds, chips, 2, count, width), BF16),
        pltpu.VMEM((width, hidden), BF16),
        pltpu.VMEM((width, hidden), BF16),
        pltpu.VMEM((hidden, width), BF16),
        pltpu.VMEM(((rows + 2) * part, group * count), BF16),
        pltpu.VMEM((chunks, (rows + 2) * part, group * count), BF16),
        pltpu.VMEM((rows * part, hidden), BF16),
        pltpu.VMEM((chunks, rows - 1, part, width), BF16),
        pltpu.VMEM((chunks, rows, part, width), BF16),
        pltpu.VMEM((chunks, rows + 2, part, width), BF16),
        pltpu.VMEM((kinds, chips, count, width), BF16),
        pltpu.VMEM((chips + 1, count, width), BF16),
        pltpu.VMEM((2, part, width), BF16),
        pltpu.VMEM((count, width), BF16),
        pltpu.VMEM((count, width), BF16),
        dma((6,)),
        dma((3,)), dma((kinds, chips)),
        dma((1,)), dma((1,)),
        dma((chips + 1,)), dma((chips, HALVES)),
        dma((1,)), dma((chips,)),
        dma((kinds, chips)), dma((chips, HALVES)), dma((chips,)),
        dma((chunks,)), dma((chunks,)),
        dma((chunks,)), dma((chunks, PIECES)),
        dma((chips + 1,)), dma((chips, PIECES)), dma((chips,)),
        dma((1,)), dma((chips + 1, PIECES)),
        dma((2,)), dma((2,)),
        dma((2,)), dma((2,)),
        dma((3,)), dma((PIECES,)), dma((1,)), dma((1,)),
    ]
    return pl.pallas_call(
        functools.partial(moe_kernel, rows, cols, slots, group, PIECES),
        out_shape=jax.ShapeDtypeStruct((count, width), BF16),
        in_specs=[any_spec] * 6,
        out_specs=pl.BlockSpec(memory_space=pl.ANY),
        scratch_shapes=scratch,
        compiler_params=pltpu.CompilerParams(
            collective_id=0, has_side_effects=True, vmem_limit_bytes=67043328
        ),
    )(expert_ids.T, gate_probs.T, tokens, w_gate, w_up, w_down)


def solution(mesh):
    in_specs = (
        P(("row", "col"), None),
        P(("row", "col"), None),
        P(("row", "col"), None),
        P(("row", "col"), None, None),
        P(("row", "col"), None, None),
        P(("row", "col"), None, None),
    )
    out_specs = P(("row", "col"), None)
    return jax.shard_map(body, mesh=mesh, in_specs=in_specs, out_specs=out_specs, check_vma=False)
```
